512 devices in a mesh: fluid: 64 (over z, x, core), solid: 8 (over y).
Axes of the slice: x: 4, y: 8, z: 8, core: 2. Of those that a mesh axis runs over, the one named last changes fastest.
Arguments:
- fluid_load: float32 [32768, 3, 128], P(('fluid', 'solid')), may hold values from -6 to 6
- stiffness: float32 [32768, 3, 128], P(('fluid', 'solid')), may hold values from 0.2 to 2
- mapping: bfloat16 [32768, 128, 128], P(('fluid', 'solid')), may hold values from -0.5 to 0.5
- live_count: int32 [512], P(('fluid', 'solid')), may hold values from 40 to 64, as said below
- dest_device: int32 [32768, 1], P(('fluid', 'solid')), may hold values from 0 to 63; in each aligned block of 64 rows (0 to 63, 64 to 127, ...) at most 2 rows name the same one
- local_block: int32 [32768], P(('fluid', 'solid')), may hold values from 0 to 3
- compliance: float32 [8, 256, 3, 128], P('solid', 'fluid'), may hold values from 0.05 to 0.5
- start_disp: float32 [8, 256, 3, 128], P('solid', 'fluid'), may hold values from -40 to 40
- residual_history: float32 [50, 8, 256, 3, 128], P(None, 'solid', 'fluid'), may hold values from -40 to 40
- update_history: float32 [50, 8, 256, 3, 128], P(None, 'solid', 'fluid'), may hold values from -2.4 to 2.4
Outputs:
- displacement: float32 [8, 256, 3, 128], P('solid', 'fluid')
- fluid_displacement: float32 [32768, 3, 128], P(('fluid', 'solid'))
The draws below stay inside these ranges and needn't reach their ends.
Inputs may be any that keep to these rules, and one draw needn't show every extreme that they name: `live_count`: each device's live blocks are its first ones; some device has exactly 64. `dest_device`: among the 64 rows of one device no fluid index appears more than 2 times.
All inputs are finite; a program needn't handle non-finite values.
Results may differ from the reference program's by a relative error of at most 0.0094.
Values may be sent and summed in bfloat16 or wider, within the bound.
No kernel may reach another device: no remote copies, remote signals or barrier semaphores. Data moves between devices by JAX's collectives and lax.ppermute only.
A program may use at most 64 MiB of HBM per device.

```python
import math
import jax
import jax.numpy as jnp
import numpy as np
from jax import lax

FB = 64
SB_DEV = 4
BF = 128
BS = 128
HIST = 50
ITERS = 2
OWN_BLK = 256
FBLK = 32768
CAP = 2
N_FLUID = 64
N_SOLID = 8


def history_pair(key):
    n_blocks = N_SOLID * OWN_BLK
    n_total = n_blocks * 3 * BS
    subkeys = jax.random.split(key, 5)
    base_draw = jax.random.normal(subkeys[0], (HIST, n_total), jnp.float32)
    shared_part = jax.random.normal(subkeys[1], (n_total,), jnp.float32)
    mixing = jnp.eye(HIST, dtype=jnp.float32) + 0.2 * jax.random.normal(subkeys[2], (HIST, HIST), jnp.float32)
    rising = 1.0 + 2.0 * jnp.arange(n_blocks, dtype=jnp.float32) / max(n_blocks - 1, 1)
    rising = jnp.repeat(rising, 3 * BS)
    basis_draw = (jnp.dot(mixing, base_draw, precision=lax.Precision.HIGHEST) + 0.5 * shared_part[None, :]) * rising[None, :]
    coef_draw = 0.15 * jax.random.normal(subkeys[3], (HIST,), jnp.float32)
    start_draw = -jnp.dot(coef_draw, basis_draw, precision=lax.Precision.HIGHEST) + 0.3 * jax.random.normal(subkeys[4], (n_total,), jnp.float32)
    basis_draw = jnp.clip(basis_draw, -40.0, 40.0).reshape(HIST, N_SOLID, OWN_BLK, 3, BS)
    start_draw = jnp.clip(start_draw, -40.0, 40.0).reshape(N_SOLID, OWN_BLK, 3, BS)
    return (basis_draw, start_draw)


def draw_residual_history(key, part):
    return history_pair(jax.random.fold_in(key, 11))[0]


def draw_start_disp(key, part):
    return history_pair(jax.random.fold_in(key, 11))[1]


def draw_live_count(key, part):
    devices_all = N_FLUID * N_SOLID
    subkeys = jax.random.split(key, 2)
    lowest = FB * 5 // 8
    first_draw = jax.random.randint(subkeys[0], (devices_all,), lowest, FB + 1)
    chosen = jax.random.randint(subkeys[1], (), 0, devices_all)
    return jnp.where(jnp.arange(devices_all) == chosen, FB, first_draw).astype(jnp.int32)


def with_ends(values, own_key, smallest, high):
    spot = [jax.random.randint(jax.random.fold_in(own_key, axis), (), 0, length) for axis, length in enumerate(values.shape)]
    widest = values.shape.index(max(values.shape))
    next_to = spot[:widest] + [(spot[widest] + 1) % values.shape[widest]] + spot[widest + 1:]
    return values.at[tuple(spot)].set(smallest).at[tuple(next_to)].set(high)


def block_levels(rng, extent, pieces, smallest, top_value):
    def one(dim, blocks):
        draws = jax.random.uniform(jax.random.fold_in(jax.random.fold_in(rng, 6), dim), (blocks,), jnp.float32, smallest / len(pieces), top_value / len(pieces))
        return jnp.repeat(jnp.exp(draws), extent[dim] // blocks).reshape((-1,) + (1,) * (len(extent) - dim - 1))

    gain = one(*pieces[0])
    for cut in pieces[1:]:
        gain = gain * one(*cut)
    return gain


def assign_block(rng, own, number, rows, amount, top, reach, lean):
    sequence = jax.random.permutation(rng, amount)
    crowded, ordinary = shares(amount, rows * top, reach, lean, True), shares(amount, rows * top, reach, lean, False)
    places = jnp.arange(amount)

    def named(lengths, turn):
        used = int((lengths > 0).sum())
        fixed = max(1, used // 4)
        moved = fixed + (places - fixed + turn * (used - fixed)) % max(1, amount - fixed)
        return jnp.zeros((amount,), jnp.int32).at[sequence[jnp.where(places < fixed, places, moved)]].set(jnp.asarray(lengths, jnp.int32))

    lengths = jnp.where(number % 4 == 0, named(crowded, number // 4), named(ordinary, number - number // 4 - 1))
    mixed = jax.random.permutation(jax.random.fold_in(own, 3), amount)
    source_of, receiver = mixed[0:amount // 2 * 2:2], mixed[1:amount // 2 * 2:2]
    margin = jnp.minimum(lengths[source_of] - 1, reach - lengths[receiver]) // 2
    margin = jnp.where((source_of == sequence[0]) | (receiver == sequence[0]) | (lengths[receiver] == 0), 0, jnp.maximum(margin, 0))
    moved = jax.random.randint(jax.random.fold_in(own, 4), (amount // 2,), 0, 1 << 20) % (margin + 1)
    lengths = lengths.at[source_of].add(-moved).at[receiver].add(moved)
    items = jnp.searchsorted(jnp.cumsum(lengths), jnp.arange(rows * top), side="right").astype(jnp.int32)
    table = items.reshape(top, rows).T
    table = table[jax.random.permutation(jax.random.fold_in(own, 1), rows)]
    turn = jax.random.randint(jax.random.fold_in(own, 2), (rows, 1), 0, top)
    return jnp.take_along_axis(table, (jnp.arange(top)[None, :] + turn) % top, axis=1)


def shares(amount, total, reach, slope, full):
    portions = [(1 << 20) // math.isqrt(rank ** slope) + 1 for rank in range(1, amount + 1)]
    largest = reach if full else min(reach, max(-(-total // amount), total * portions[0] // sum(portions)))
    least = 1 if total - largest >= amount - 1 else 0
    given, surplus = [largest] + [least] * (amount - 1), total - largest - least * (amount - 1)
    while surplus > 0:
        free = [i for i in range(1, amount) if given[i] < largest] or [i for i in range(1, amount) if given[i] < reach]
        whole, remaining = sum([portions[i] for i in free]), surplus
        for i in free:
            addition = min(reach - given[i], max(1, remaining * portions[i] // whole), surplus)
            given[i] = given[i] + addition
            surplus = surplus - addition
    return np.array(given)


def centred(rng, extent, spread, bound, pieces=(), kind=jnp.bfloat16):
    level = block_levels(rng, extent, pieces, -0.22, 0.18) if pieces else 1.0
    result = jax.random.normal(rng, extent, jnp.float32) * spread * level
    return jnp.minimum(jnp.maximum(result, -bound), bound).astype(kind)


def setup_inputs(seed: int = 0) -> dict:
    keys = jax.random.split(jax.random.key(seed), 11)
    fluid_load = centred(keys[0], (FBLK, 3, BF), 1.0, 6.0, ((0, 512),), jnp.float32)
    stiffness = jnp.clip(jnp.exp(math.log(2.0) - 2.3025851 * jax.random.uniform(keys[1], (FBLK, 3, BF), jnp.float32) ** block_levels(keys[1], (FBLK, 3, BF), ((0, 512),), -0.2, 0.2)), 0.2, 2.0)
    mapping = centred(keys[2], (FBLK, BS, BF), BF ** -0.5, 0.5, ((0, 512),))
    live_count = draw_live_count(jax.random.fold_in(keys[10], 71), 0)
    dest_device_keys = jax.random.split(jax.random.fold_in(keys[4], 1), FBLK // FB)
    dest_device_turns = jax.random.permutation(jax.random.fold_in(keys[4], 3), FBLK // FB)
    dest_device = jax.vmap(lambda own, number: assign_block(jax.random.fold_in(keys[4], 2), own, number, FB, N_FLUID, 1, CAP, 0))(dest_device_keys, dest_device_turns).reshape((FBLK, 1))
    local_block = with_ends(jax.random.randint(keys[5], (FBLK,), 0, SB_DEV), jax.random.fold_in(keys[5], 1), 0, SB_DEV - 1).astype(jnp.int32)
    compliance = jnp.clip(jnp.exp(math.log(0.5) - 2.3025851 * jax.random.uniform(keys[6], (N_SOLID, OWN_BLK, 3, BS), jnp.float32) ** block_levels(keys[6], (N_SOLID, OWN_BLK, 3, BS), ((0, 8), (1, 64)), -0.2, 0.2)), 0.05, 0.5)
    start_disp = draw_start_disp(jax.random.fold_in(keys[10], 71), 0)
    residual_history = draw_residual_history(jax.random.fold_in(keys[10], 71), 0)
    update_history = centred(keys[9], (HIST, N_SOLID, OWN_BLK, 3, BS), 0.3, 2.4, ((1, 8), (2, 64)), jnp.float32)
    return dict(fluid_load=fluid_load, stiffness=stiffness, mapping=mapping, live_count=live_count, dest_device=dest_device, local_block=local_block, compliance=compliance, start_disp=start_disp, residual_history=residual_history, update_history=update_history)


ridge_share = 0.01

def solve_small(gram_matrix, right_side):
    order = gram_matrix.shape[0]
    ridge = ridge_share * jnp.trace(gram_matrix) / order
    factor = jnp.linalg.cholesky(gram_matrix + ridge * jnp.eye(order, dtype=gram_matrix.dtype))
    halfway = lax.linalg.triangular_solve(factor, right_side[:, None], left_side=True, lower=True)
    solved = lax.linalg.triangular_solve(factor, halfway, left_side=True, lower=True, transpose_a=True)
    return -solved[:, 0]

def reference(fluid_load, stiffness, mapping, live_count, dest_device, local_block, compliance, start_disp, residual_history, update_history):
    devices_all = N_FLUID * N_SOLID
    block_ids = jnp.arange(FBLK, dtype=jnp.int32)
    device_of = block_ids // FB
    alive = (block_ids % FB < live_count[device_of]).astype(jnp.float32)[:, None, None]
    target = (device_of % N_SOLID * OWN_BLK + dest_device[:, 0] * SB_DEV + local_block).astype(jnp.int32)
    mapping_dev = mapping.reshape(devices_all, FB, BS, BF)
    target_dev = target.reshape(devices_all, FB)

    def to_fluid(struct_disp):
        packed = struct_disp.astype(jnp.bfloat16).reshape(N_SOLID * OWN_BLK, 3, BS)

        def apply_back(scan_item):
            block_map, block_target = scan_item
            picked = packed[block_target]
            return jnp.einsum('bjn,bcj->bcn', block_map.astype(jnp.float32), picked.astype(jnp.float32))
        fluid_disp = lax.map(apply_back, (mapping_dev, target_dev)).reshape(FBLK, 3, BF)
        return fluid_disp * alive

    def to_solid(fluid_disp):
        fluid_force = (alive * (fluid_load - stiffness * fluid_disp)).astype(jnp.bfloat16)
        fluid_force = fluid_force.reshape(devices_all, FB, 3, BF)

        def accumulate(summed, scan_item):
            block_map, block_force, block_target = scan_item
            contrib = jnp.einsum('bjn,bcn->bcj', block_map.astype(jnp.float32), block_force.astype(jnp.float32))
            return (summed.at[block_target].add(contrib), None)
        summed0 = jnp.zeros((N_SOLID * OWN_BLK, 3, BS), jnp.float32)
        summed, _ = lax.scan(accumulate, summed0, (mapping_dev, fluid_force, target_dev))
        return summed.reshape(N_SOLID, OWN_BLK, 3, BS)
    struct_disp = start_disp
    basis_cols = residual_history
    updates = update_history
    last_resid = struct_disp
    last_image = struct_disp
    for iteration in range(ITERS):
        fluid_disp = to_fluid(struct_disp)
        struct_image = compliance * to_solid(fluid_disp)
        residual = struct_image - struct_disp
        if iteration > 0:
            basis_cols = jnp.concatenate([basis_cols[1:], (residual - last_resid)[None]], 0)
            updates = jnp.concatenate([updates[1:], (struct_image - last_image)[None]], 0)
        basis_flat = basis_cols.reshape(HIST, -1)
        resid_flat = residual.reshape(-1)
        gram_matrix = jnp.dot(basis_flat, basis_flat.T, precision=lax.Precision.HIGHEST)
        right_side = jnp.dot(basis_flat, resid_flat, precision=lax.Precision.HIGHEST)
        coefficients = solve_small(gram_matrix, right_side)
        struct_disp = struct_image + jnp.tensordot(coefficients, updates, axes=1, precision=lax.Precision.HIGHEST)
        last_resid = residual
        last_image = struct_image
    final_disp = to_fluid(struct_disp)
    return (struct_disp, final_disp)
```

```python
import jax
import jax.numpy as jnp
from jax import lax
from jax.experimental import pallas as pl
from jax.experimental.pallas import tpu as pltpu
from jax.sharding import Mesh
from jax.sharding import PartitionSpec as P

ITERS = 2
HIST = 50
RIDGE_SHARE = 0.01
ALL = ("z", "x", "c", "solid")
FLUID = ("z", "x", "c")
NEAR = ("c", "solid")
FAR = ("z", "x")
ROWS = 56
RHS = 64
HIGHEST = lax.Precision.HIGHEST


def exchange(x, axes):
    return lax.all_to_all(x, axes, split_axis=0, concat_axis=0, tiled=True)


def sent_to_all(x, axes):
    return exchange(jnp.broadcast_to(x, (lax.axis_size(axes), *x.shape)), axes)


def three_pieces(x):
    high = lax.reduce_precision(x, 8, 7)
    rest = x - high
    middle = lax.reduce_precision(rest, 8, 7)
    return high, middle, rest - middle


def solve_kernel(system_ref, out_ref):
    a = system_ref[...]
    rows = lax.broadcasted_iota(jnp.int32, a.shape, 0)
    lanes = lax.broadcasted_iota(jnp.int32, a.shape, 1)
    diag = (rows == lanes) & (rows < HIST)
    trace = jnp.sum(jnp.where(diag, a, 0.0))
    a = a + jnp.where(diag, RIDGE_SHARE * trace / HIST, 0.0)
    for k in range(HIST):
        row = a[k : k + 1, :]
        row = row / row[:, k : k + 1]
        a = jnp.where(rows == k, row, a - a[:, k : k + 1] * row)
    out_ref[...] = -jnp.broadcast_to(a[:, RHS : RHS + 1], a.shape)


def solve_small(gram_matrix, right_side):
    system = jnp.zeros((ROWS, 128), jnp.float32)
    system = system.at[:HIST, :HIST].set(gram_matrix)
    system = system.at[:HIST, RHS].set(right_side)
    solved = pl.pallas_call(
        solve_kernel,
        out_shape=jax.ShapeDtypeStruct((ROWS, 128), jnp.float32),
        in_specs=[pl.BlockSpec(memory_space=pltpu.VMEM)],
        out_specs=pl.BlockSpec(memory_space=pltpu.VMEM),
        name="solve",
    )(system)
    return solved[:HIST, 0]


def body(
    fluid_load,
    stiffness,
    mapping,
    live_count,
    dest_device,
    local_block,
    compliance,
    start_disp,
    residual_history,
    update_history,
):
    blocks = mapping.shape[0]
    sub_blocks = compliance.shape[1]
    peers = lax.axis_size(FLUID)
    far = lax.axis_size(FAR)
    near = lax.axis_size(NEAR)
    alive = (jnp.arange(blocks) < live_count[0]).astype(jnp.float32)[:, None, None]
    dest = dest_device[:, 0]
    order = jnp.arange(blocks)
    earlier = (dest[:, None] == dest[None, :]) & (order[None, :] < order[:, None])
    place = dest * 2 + jnp.sum(earlier, axis=1)
    place_hot = (place[:, None] == jnp.arange(2 * peers)[None, :]).astype(jnp.bfloat16)
    names = jnp.sum(
        jnp.where(
            place[:, None] == jnp.arange(2 * peers)[None, :], local_block[:, None] + 1, 0
        ),
        axis=0,
    ).astype(jnp.float32)

    def on_fluid(picked):
        return jnp.einsum(
            "bjn,bcj->bcn",
            mapping,
            picked.astype(jnp.bfloat16),
            preferred_element_type=jnp.float32,
        ) * alive

    def places_filled(picked):
        force = (alive * (fluid_load - stiffness * on_fluid(picked))).astype(jnp.bfloat16)
        contrib = jnp.einsum("bjn,bcn->bcj", mapping, force, preferred_element_type=jnp.float32)
        filled = jnp.einsum(
            "bp,bcj->pcj",
            place_hot,
            contrib.astype(jnp.bfloat16),
            preferred_element_type=jnp.float32,
        )
        return filled.astype(jnp.bfloat16).reshape(peers, 6, 128)

    def summed_at_owner(got, names_hot):
        return jnp.einsum(
            "pk,pcj->kcj",
            names_hot,
            got[:, :6].reshape(2 * peers, 3, 128),
            preferred_element_type=jnp.float32,
        )[None]

    def picked_by_places(struct_disp, names_hot):
        packed = struct_disp[0].astype(jnp.bfloat16)
        chosen = jnp.einsum(
            "pk,kcj->pcj", names_hot, packed, preferred_element_type=jnp.float32
        ).astype(jnp.bfloat16)
        got = exchange(chosen.reshape(peers, 6, 128), FLUID)
        return jnp.einsum(
            "bp,pcj->bcj",
            place_hot,
            got.reshape(2 * peers, 3, 128),
            preferred_element_type=jnp.float32,
        )

    basis = residual_history.reshape(HIST, -1)
    gram_local = jnp.dot(basis, basis.T, precision=HIGHEST)
    pieces = three_pieces(jnp.pad(gram_local, ((0, peers - HIST), (0, 64 - HIST))))
    side = jnp.concatenate(
        [pieces[0], pieces[1], pieces[2], jnp.zeros((peers, 62)), names.reshape(peers, 2)], axis=1
    )
    side = side.astype(jnp.bfloat16).reshape(peers, 2, 128)

    whole = sent_to_all(start_disp[0].astype(jnp.bfloat16).reshape(sub_blocks, 3 * 128), FLUID)
    target = dest * sub_blocks + local_block
    target_hot = (target[:, None] == jnp.arange(peers * sub_blocks)[None, :]).astype(jnp.bfloat16)
    picked = jnp.dot(
        target_hot,
        whole.reshape(peers * sub_blocks, 3 * 128),
        preferred_element_type=jnp.float32,
    ).reshape(blocks, 3, 128)

    got = exchange(jnp.concatenate([places_filled(picked), side], axis=1), FLUID)
    names_got = got[:, 7, 126:].reshape(2 * peers)
    names_hot = (
        names_got[:, None] == jnp.arange(1, sub_blocks + 1).astype(jnp.bfloat16)[None, :]
    ).astype(jnp.bfloat16)
    row_pieces = jnp.sum(got[:, 6:8].astype(jnp.float32), axis=0)
    gram_row = row_pieces[0, :64] + row_pieces[0, 64:] + row_pieces[1, :64]
    gram_row = jnp.where(jnp.arange(64) < HIST, gram_row, 0.0)

    image = compliance * summed_at_owner(got, names_hot)
    residual = image - start_disp
    right_local = jnp.dot(basis, residual.reshape(-1), precision=HIGHEST)
    line = jnp.concatenate([jnp.pad(right_local, (0, 64 - HIST)), gram_row])
    near_got = sent_to_all(line, NEAR).reshape(2, near // 2, 128)
    near_rows = jnp.sum(near_got[:, :, 64:], axis=1).reshape(1, 128)
    near_right = jnp.sum(near_got, axis=(0, 1))[None]
    far_got = sent_to_all(jnp.concatenate([near_right, near_rows], axis=0), FAR)
    gram = far_got[:, 1].reshape(peers, 64)[:HIST, :HIST]
    right = jnp.sum(far_got[:, 0, :HIST], axis=0)
    coefficients = solve_small(gram, right)
    struct_disp = image + jnp.tensordot(coefficients, update_history, axes=1, precision=HIGHEST)

    filled = places_filled(picked_by_places(struct_disp, names_hot))
    got = exchange(filled, FLUID)
    last_image, last_residual = image, residual
    image = compliance * summed_at_owner(got, names_hot)
    residual = image - struct_disp
    newest = residual - last_residual
    both = jnp.stack([residual.reshape(-1), newest.reshape(-1)])
    columns = jnp.concatenate([basis[1:], newest.reshape(1, -1)], axis=0)
    sums = jnp.pad(jnp.dot(both, columns.T, precision=HIGHEST), ((0, 0), (0, 64 - HIST)))
    near_got = sent_to_all(sums.reshape(1, 128), NEAR)
    far_got = sent_to_all(jnp.sum(near_got, axis=0), FAR)
    sums = jnp.sum(far_got, axis=0).reshape(2, 64)[:, :HIST]
    right, row = sums[0], sums[1]
    gram = jnp.concatenate(
        [jnp.concatenate([gram[1:, 1:], row[:-1, None]], 1), row[None, :]], 0
    )
    coefficients = solve_small(gram, right)
    struct_disp = (
        image
        + jnp.tensordot(coefficients[:-1], update_history[1:], axes=1, precision=HIGHEST)
        + coefficients[-1] * (image - last_image)
    )
    final_disp = on_fluid(picked_by_places(struct_disp, names_hot))
    return (struct_disp, final_disp)


def solution(mesh):
    split = Mesh(mesh.devices.reshape(8, 4, 2, mesh.shape["solid"]), ALL)
    in_specs = (
        P(ALL, None, None),
        P(ALL, None, None),
        P(ALL, None, None),
        P(ALL),
        P(ALL, None),
        P(ALL),
        P("solid", FLUID, None, None),
        P("solid", FLUID, None, None),
        P(None, "solid", FLUID, None, None),
        P(None, "solid", FLUID, None, None),
    )
    out_specs = (P("solid", FLUID, None, None), P(ALL, None, None))
    return jax.shard_map(body, mesh=split, in_specs=in_specs, out_specs=out_specs, check_vma=False)
```

```python
import jax
import jax.numpy as jnp
from jax import lax
from jax.experimental import pallas as pl
from jax.experimental.pallas import tpu as pltpu
from jax.sharding import Mesh
from jax.sharding import PartitionSpec as P

HIST = 50
RIDGE_SHARE = 0.01
ALL = ("z", "x", "c", "solid")
FLUID = ("z", "x", "c")
NEAR = ("c", "solid")
FAR = ("z", "x")
COLS = 56
PARTS = 12
WIDE = 64
F32, BF16 = jnp.float32, jnp.bfloat16
HIGHEST = lax.Precision.HIGHEST
VMEM = pl.BlockSpec(memory_space=pltpu.VMEM)
SMEM = pl.BlockSpec(memory_space=pltpu.SMEM)


def exchange(x, axes):
    return lax.all_to_all(x, axes, split_axis=0, concat_axis=0, tiled=True)


def three_pieces(x):
    high = lax.reduce_precision(x, 8, 7)
    rest = x - high
    middle = lax.reduce_precision(rest, 8, 7)
    return high, middle, rest - middle


def call(kernel, name, outs, *args, in_specs=None, scratch=()):
    return pl.pallas_call(
        kernel,
        out_shape=[jax.ShapeDtypeStruct(shape, dtype) for shape, dtype in outs],
        in_specs=in_specs or [VMEM] * len(args),
        out_specs=[VMEM] * len(outs),
        scratch_shapes=list(scratch),
        name=name,
    )(*args)


def dot(a, b, dims=((1,), (0,)), precision=None):
    return lax.dot_general(a, b, (dims, ((), ())), precision=precision, preferred_element_type=F32)


def forces_kernel(x_ref, pick_ref, back_ref, map_ref, load_ref, stiff_ref, side_ref, out_ref, xs, fs, cs):
    blocks = map_ref.shape[0]
    xs[...] = dot(pick_ref[...], x_ref[...].reshape(pick_ref.shape[1], 128))
    for b in range(blocks):
        rows = slice(8 * b, 8 * b + 8)
        u = dot(xs[rows, :].astype(BF16), map_ref[b])
        fs[rows, :] = load_ref[rows, :] - stiff_ref[rows, :] * u
    for b in range(blocks):
        rows = slice(8 * b, 8 * b + 8)
        cs[rows, :] = dot(fs[rows, :].astype(BF16), map_ref[b], ((1,), (1,)))
    filled = dot(back_ref[...], cs[...].astype(BF16))
    out_ref[...] = (filled.reshape(out_ref.shape) + side_ref[...].astype(F32)).astype(BF16)


def final_kernel(live_ref, x_ref, pick_ref, map_ref, out_ref, xs):
    xs[...] = dot(pick_ref[...], x_ref[...].reshape(pick_ref.shape[1], 128))
    for b in range(map_ref.shape[0]):
        u = dot(xs[8 * b : 8 * b + 8, :].astype(BF16), map_ref[b])
        out_ref[b] = u[:3] * jnp.where(b < live_ref[0], 1.0, 0.0)


def lanes_of(shape):
    return lax.broadcasted_iota(jnp.int32, shape, len(shape) - 1)


def rows_of(shape):
    return lax.broadcasted_iota(jnp.int32, shape, 0)


def history_sums(vr_ref, vector):
    acc = vr_ref[0] * vector[0:1, :]
    for m in range(1, PARTS):
        acc = acc + vr_ref[m] * vector[m : m + 1, :]
    return acc


def as_row(first, second):
    gap = jnp.zeros((WIDE - COLS, 128), F32)
    stacked = jnp.concatenate([first, gap, second, gap], axis=0)
    return dot(jnp.ones((8, 128), F32), stacked, ((1,), (1,)), HIGHEST)[0:1, :]


def owner_first_kernel(got_ref, comp_ref, x_ref, vr_ref, msg_ref, image_ref, resid_ref, q_ref, qt_ref, xs):
    xs[...] = got_ref[...].astype(F32).reshape(512, 128)
    mark6 = xs[pl.ds(6, 64, stride=8), :]
    mark7 = xs[pl.ds(7, 64, stride=8), :]
    sum6 = jnp.sum(mark6, axis=0, keepdims=True)
    sum7 = jnp.sum(mark7, axis=0, keepdims=True)
    gram_row = sum6 + pltpu.roll(sum6, WIDE, 1) + pltpu.roll(sum7, WIDE, 1)
    spread = (lanes_of((64, 512)) // 8 == rows_of((64, 512))).astype(BF16)
    wide = dot(mark7.astype(BF16), spread, ((0,), (0,)))
    part = rows_of((16, 512))
    row = lanes_of((16, 512)) % 8
    match = part % 3 == row % 3
    q = jnp.where(match & (row < 3), wide[64:80], 0.0)
    q = q + jnp.where(match & (row >= 3) & (row < 6), wide[80:96], 0.0)
    q = q.astype(BF16)
    q_ref[...] = q
    tall = jnp.broadcast_to(
        xs[...].reshape(64, 8, 128)[:, 7:8, :], (64, 8, 128)
    ).reshape(512, 128)
    lane = lanes_of((512, 128))
    row = rows_of((512, 128)) % 8
    match = ((lane % 16) % 3 == row % 3) & (lane % 16 < PARTS)
    match = match & (((row < 3) & (lane // 16 == 4)) | ((row >= 3) & (row < 6) & (lane // 16 == 5)))
    qt_ref[...] = jnp.where(match, tall, 0.0).astype(BF16)
    image = comp_ref[...] * dot(q, xs[...].astype(BF16))
    resid = image - x_ref[...]
    image_ref[...] = image
    resid_ref[...] = resid
    sums = history_sums(vr_ref, resid)
    line = as_row(sums, jnp.zeros_like(sums))
    line = jnp.where(lanes_of(line.shape) < WIDE, line, gram_row)
    msg_ref[...] = jnp.broadcast_to(line.reshape(1, 1, 128), msg_ref.shape)


def owner_next_kernel(got_ref, q_ref, comp_ref, x_ref, last_ref, vr_ref, msg_ref, image_ref):
    got = got_ref[...].astype(F32).reshape(512, 128).astype(BF16)
    image = comp_ref[...] * dot(q_ref[...], got)
    image_ref[...] = image
    resid = image - x_ref[...]
    newest = resid - last_ref[...]
    first = rows_of((COLS, 128)) == 0
    own_right = jnp.sum(newest * resid, axis=0, keepdims=True)
    own_row = jnp.sum(newest * newest, axis=0, keepdims=True)
    right = jnp.where(first, own_right, history_sums(vr_ref, resid))
    row = jnp.where(first, own_row, history_sums(vr_ref, newest))
    line = as_row(right, row)
    msg_ref[...] = jnp.broadcast_to(line.reshape(1, 1, 128), msg_ref.shape)


def near_first_kernel(in_ref, out_ref):
    sums = []
    for c in range(2):
        total = in_ref[8 * c]
        for y in range(1, 8):
            total = total + in_ref[8 * c + y]
        sums.append(total)
    right = sums[0] + sums[1]
    rows = jnp.where(lanes_of((1, 128)) < WIDE, pltpu.roll(sums[0], WIDE, 1), sums[1])
    both = jnp.concatenate([right, rows], axis=0)
    out_ref[...] = jnp.broadcast_to(both[None], out_ref.shape)


def near_next_kernel(in_ref, out_ref):
    total = in_ref[0]
    for i in range(1, in_ref.shape[0]):
        total = total + in_ref[i]
    out_ref[...] = jnp.broadcast_to(total[None], out_ref.shape)


def as_column(row, shape):
    on_diag = lanes_of(shape) == rows_of(shape)
    return jnp.sum(jnp.where(on_diag, row, 0.0), axis=1, keepdims=True)


def solved(gram, right):
    lanes, rows = lanes_of(gram.shape), rows_of(gram.shape)
    diag = (rows == lanes) & (rows < HIST)
    trace = jnp.sum(jnp.where(diag, gram, 0.0))
    a = gram + jnp.where(diag, RIDGE_SHARE * trace / HIST, 0.0)
    a = jnp.where(lanes == WIDE, as_column(right, gram.shape), a)
    for k in range(HIST):
        row = a[k : k + 1, :]
        row = row / row[:, k : k + 1]
        a = jnp.where(rows == k, row, a - a[:, k : k + 1] * row)
    return -jnp.broadcast_to(a[:, WIDE : WIDE + 1], a.shape)


def moved(image, coefficients, column):
    lines = [jnp.sum(coefficients * column(m), axis=0, keepdims=True) for m in range(PARTS)]
    return image + jnp.concatenate([*lines, jnp.zeros((16 - PARTS, 128), F32)], axis=0)


def chosen(x, qt):
    tall = jnp.concatenate(
        [jnp.zeros((WIDE, 128), F32), x, x, jnp.zeros((32, 128), F32)], axis=0
    )
    return dot(qt, tall.astype(BF16)).astype(BF16)


def far_first_kernel(in_ref, image_ref, wr_ref, qt_ref, send_ref, x_ref, gram_ref, gs):
    right = in_ref[0, 0:1, :]
    gs[0:1, :] = in_ref[0, 1:2, :]
    for i in range(1, 32):
        right = right + in_ref[i, 0:1, :]
        gs[i : i + 1, :] = in_ref[i, 1:2, :]
    half = gs[...]
    gram = jnp.concatenate([half, pltpu.roll(half, WIDE, 1)], axis=0)[:COLS]
    gram = jnp.where(lanes_of(gram.shape) < WIDE, gram, 0.0)
    gram_ref[...] = gram
    coefficients = solved(gram, right)
    x = moved(image_ref[...], coefficients, lambda m: wr_ref[m])
    x_ref[...] = x
    send_ref[...] = chosen(x, qt_ref[...]).astype(F32).reshape(send_ref.shape).astype(BF16)


def far_next_kernel(in_ref, gram_ref, image_ref, last_ref, wr_ref, qt_ref, send_ref, x_ref):
    total = in_ref[0]
    for i in range(1, 32):
        total = total + in_ref[i]
    gram = gram_ref[...]
    lanes, rows = lanes_of(gram.shape), rows_of(gram.shape)
    new_row = jnp.where(lanes_of(total.shape) < WIDE, pltpu.roll(total, WIDE, 1), 0.0)
    gram = jnp.where(rows == 0, new_row, gram)
    gram = jnp.where(lanes == 0, as_column(new_row, gram.shape), gram)
    coefficients = solved(gram, total)
    image = image_ref[...]
    step = image - last_ref[...]
    first = rows_of((COLS, 128)) == 0
    x = moved(image, coefficients, lambda m: jnp.where(first, step[m : m + 1, :], wr_ref[m]))
    for m in range(PARTS):
        x_ref[0, m // 3, m % 3 : m % 3 + 1, :] = x[m : m + 1, :]
    send_ref[...] = chosen(x, qt_ref[...]).astype(F32).reshape(send_ref.shape).astype(BF16)


def body(
    fluid_load,
    stiffness,
    mapping,
    live_count,
    dest_device,
    local_block,
    compliance,
    start_disp,
    residual_history,
    update_history,
):
    blocks = mapping.shape[0]
    sub_blocks = compliance.shape[1]
    peers = lax.axis_size(FLUID)
    near, far = lax.axis_size(NEAR), lax.axis_size(FAR)
    message = (peers, 8, 128)

    packed = jnp.swapaxes(start_disp[0].astype(BF16), 0, 1)
    whole = exchange(jnp.broadcast_to(packed, (peers, *packed.shape)), FLUID)

    dest = dest_device[:, 0]
    order = jnp.arange(blocks)
    earlier = (dest[:, None] == dest[None, :]) & (order[None, :] < order[:, None])
    slot = jnp.sum(earlier, axis=1)
    component = jnp.arange(8)
    column = dest[:, None] * 8 + slot[:, None] * 3 + component
    column = jnp.where(component < 3, column, -1).reshape(8 * blocks)
    whole_column = dest[:, None] * PARTS + component * sub_blocks + local_block[:, None]
    whole_column = jnp.where(component < 3, whole_column, -1).reshape(8 * blocks)
    pick = (column[:, None] == jnp.arange(8 * peers)[None, :]).astype(BF16)
    back = (jnp.arange(8 * peers)[:, None] == column[None, :]).astype(BF16)
    pick_whole = (whole_column[:, None] == jnp.arange(PARTS * peers)[None, :]).astype(BF16)
    alive = (order < live_count[0]).astype(F32)[:, None, None]
    load8 = jnp.pad(alive * fluid_load, ((0, 0), (0, 5), (0, 0))).reshape(8 * blocks, 128)
    stiff8 = jnp.pad(alive * stiffness, ((0, 0), (0, 5), (0, 0))).reshape(8 * blocks, 128)
    place = dest * 2 + slot
    names = jnp.sum(
        jnp.where(place[:, None] == jnp.arange(2 * peers)[None, :], local_block[:, None] + 1, 0), axis=0
    ).reshape(peers, 2, 1)
    part = jnp.arange(16)
    marks = ((names == part // 3 + 1) & (part < PARTS)).astype(F32).reshape(peers, 32)
    columns_first = lambda h: jnp.pad(
        jnp.moveaxis(h.reshape(HIST, PARTS, 128), 0, 1), ((0, 0), (0, COLS - HIST), (0, 0))
    )
    vr, wr = columns_first(residual_history), columns_first(update_history)
    basis = residual_history.reshape(HIST, -1)
    gram_local = jnp.pad(
        jnp.dot(basis, basis.T, precision=HIGHEST), ((0, peers - HIST), (0, WIDE - HIST))
    )
    gram_local = jnp.swapaxes(gram_local.reshape(2, far, WIDE), 0, 1).reshape(peers, WIDE)
    high, middle, low = three_pieces(gram_local)
    side = jnp.concatenate([high, middle, low, marks, jnp.zeros((peers, 32))], axis=1)
    side = jnp.pad(side.astype(BF16).reshape(peers, 2, 128), ((0, 0), (6, 0), (0, 0)))
    rows = lambda a: jnp.pad(a.reshape(PARTS, 128), ((0, 16 - PARTS), (0, 0)))
    comp, x = rows(compliance), rows(start_disp)

    square = pltpu.VMEM((8 * blocks, 128), F32)
    forces = lambda *args: call(
        forces_kernel, "forces", [(message, BF16)], *args, scratch=[square, square, square]
    )[0]
    sent = forces(whole.reshape(-1, 128), pick_whole, back, mapping, load8, stiff8, side)
    got = exchange(sent, FLUID)
    line, image, resid, q, qt = call(
        owner_first_kernel,
        "owner_first",
        [((near, 1, 128), F32), ((16, 128), F32), ((16, 128), F32), ((16, 8 * peers), BF16), ((8 * peers, 128), BF16)],
        got,
        comp,
        x,
        vr,
        scratch=[square],
    )
    line = exchange(line, NEAR)
    line = call(near_first_kernel, "near_first", [((far, 2, 128), F32)], line)[0]
    line = exchange(line, FAR)
    sent, x, gram = call(
        far_first_kernel,
        "far_first",
        [(message, BF16), ((16, 128), F32), ((COLS, 128), F32)],
        line,
        image,
        wr,
        qt,
        scratch=[pltpu.VMEM((far, 128), F32)],
    )

    got = exchange(sent, FLUID)
    sent = forces(got, pick, back, mapping, load8, stiff8, jnp.zeros_like(side))
    got = exchange(sent, FLUID)
    last_image = image
    line, image = call(
        owner_next_kernel,
        "owner_next",
        [((near, 1, 128), F32), ((16, 128), F32)],
        got,
        q,
        comp,
        x,
        resid,
        vr,
    )
    line = exchange(line, NEAR)
    line = call(near_next_kernel, "near_next", [((far, 1, 128), F32)], line)[0]
    line = exchange(line, FAR)
    sent, struct_disp = call(
        far_next_kernel,
        "far_next",
        [(message, BF16), (start_disp.shape, F32)],
        line,
        gram,
        image,
        last_image,
        wr,
        qt,
    )
    got = exchange(sent, FLUID)
    final_disp = call(
        final_kernel,
        "final",
        [(fluid_load.shape, F32)],
        live_count,
        got,
        pick,
        mapping,
        in_specs=[SMEM, VMEM, VMEM, VMEM],
        scratch=[square],
    )[0]
    return (struct_disp, final_disp)


def solution(mesh):
    split = Mesh(mesh.devices.reshape(8, 4, 2, mesh.shape["solid"]), ALL)
    in_specs = (
        P(ALL, None, None),
        P(ALL, None, None),
        P(ALL, None, None),
        P(ALL),
        P(ALL, None),
        P(ALL),
        P("solid", FLUID, None, None),
        P("solid", FLUID, None, None),
        P(None, "solid", FLUID, None, None),
        P(None, "solid", FLUID, None, None),
    )
    out_specs = (P("solid", FLUID, None, None), P(ALL, None, None))
    return jax.shard_map(body, mesh=split, in_specs=in_specs, out_specs=out_specs, check_vma=False)
```

```python
import jax
import jax.numpy as jnp
from jax import lax
from jax.experimental import pallas as pl
from jax.experimental.pallas import tpu as pltpu
from jax.sharding import Mesh
from jax.sharding import PartitionSpec as P

HIST = 50
RIDGE_SHARE = 0.01
ALL = ("z", "x", "c", "solid")
FLUID = ("z", "x", "c")
NEAR = ("c", "solid")
FAR = ("z", "x")
COLS = 56
PARTS = 12
WIDE = 64
F32, BF16 = jnp.float32, jnp.bfloat16
HIGHEST = lax.Precision.HIGHEST
VMEM = pl.BlockSpec(memory_space=pltpu.VMEM)
SMEM = pl.BlockSpec(memory_space=pltpu.SMEM)


def exchange(x, axes):
    return lax.all_to_all(x, axes, split_axis=0, concat_axis=0, tiled=True)


def call(kernel, name, outs, *args, in_specs=None, scratch=(), mib=2, cost=None):
    return pl.pallas_call(
        kernel,
        out_shape=[jax.ShapeDtypeStruct(shape, dtype) for shape, dtype in outs],
        compiler_params=pltpu.CompilerParams(vmem_limit_bytes=mib << 20),
        in_specs=in_specs or [VMEM] * len(args),
        out_specs=[VMEM] * len(outs),
        scratch_shapes=list(scratch),
        cost_estimate=cost,
        name=name,
    )(*args)


def dot(a, b, dims=((1,), (0,)), precision=None):
    return lax.dot_general(a, b, (dims, ((), ())), precision=precision, preferred_element_type=F32)


def lanes_of(shape):
    return lax.broadcasted_iota(jnp.int32, shape, len(shape) - 1)


def rows_of(shape):
    return lax.broadcasted_iota(jnp.int32, shape, 0)


def every(ref, part):
    return ref[pl.ds(part, HIST, stride=PARTS), :]


def as_column(row, shape):
    on_diag = lanes_of(shape) == rows_of(shape)
    return jnp.sum(jnp.where(on_diag, row, jnp.zeros_like(row)), axis=1, keepdims=True)


def spread_kernel(live_ref, x_ref, out_ref, alive_ref):
    alive_ref[...] = jnp.where(rows_of(alive_ref.shape) < live_ref[0], 1.0, 0.0)
    out_ref[...] = jnp.broadcast_to(x_ref[...].astype(BF16)[None], out_ref.shape)


def forces_first_kernel(
    alive_ref, x_ref, dest_ref, local_ref, hist_ref, raw_load_ref, raw_stiff_ref, map_ref, comp_ref, start_ref,
    out_ref, pick_ref, back_ref, load_ref, stiff_ref, flat_comp_ref, flat_start_ref, gs, ss, whole_ref, xs, us,
):
    for c in range(3):
        flat_comp_ref[4 * c : 4 * c + 4, :] = comp_ref[c]
        flat_start_ref[4 * c : 4 * c + 4, :] = start_ref[c]
    square = (64, 128)
    lanes, rows = lanes_of(square), rows_of(square)
    dest = jnp.where(lanes < 64, jnp.concatenate([dest_ref[...]] * 2, axis=1), -1)
    local = jnp.concatenate([local_ref[...]] * 2, axis=1)
    dest_column = as_column(dest.astype(F32), square)
    local_column = as_column(local.astype(F32), square).astype(jnp.int32)
    same = (dest_column == dest.astype(F32)) & (lanes < 64)
    dest_column = dest_column.astype(jnp.int32)
    slot_column = jnp.sum(jnp.where(same & (lanes < rows), 1.0, 0.0), axis=1, keepdims=True)
    slot_row = jnp.sum(jnp.where(same & (rows < lanes), 1.0, 0.0), axis=0, keepdims=True)
    slot_column = slot_column.astype(jnp.int32)
    place_column = dest_column * 8 + slot_column * 4
    place_row = dest[0:1] * 8 + slot_row.astype(jnp.int32) * 4
    wide = lanes_of((64, 512))
    wider = lanes_of((64, 768))
    for c in range(3):
        pick_ref[64 * c : 64 * c + 64, :] = jnp.where(wide == place_column + c, 1.0, 0.0).astype(BF16)
        whole_column = dest_column * PARTS + 4 * c + local_column
        whole_ref[64 * c : 64 * c + 64, :] = jnp.where(wider == whole_column, 1.0, 0.0).astype(BF16)
    tall = rows_of((512, 128))
    low = lanes[0:1] < 64
    first = jnp.where(low, place_row, pltpu.roll(place_row, 64, 1) + 1)
    second = jnp.where(low, place_row + 2, -1)
    back_ref[:, 0:128] = jnp.where(tall == first, 1.0, 0.0).astype(BF16)
    back_ref[:, 128:256] = jnp.where(tall == second, 1.0, 0.0).astype(BF16)
    part = lanes % 16
    held = (lanes >= 64) & (lanes // 16 - 4 == slot_column) & (part % 4 == local_column) & (part < PARTS)
    onto = jnp.where(dest == rows, 1.0, 0.0).astype(BF16)
    marks = dot(onto[:, 0:64], jnp.where(held, 1.0, 0.0).astype(BF16))
    history = jnp.concatenate([every(hist_ref, m) for m in range(PARTS)], axis=1)
    gs[...] = jnp.zeros(square, F32)
    gs[0:HIST, 0:HIST] = dot(history, history, ((1,), (1,)), HIGHEST)
    gram = gs[...]
    high = gram.astype(BF16).astype(F32)
    middle = (gram - high).astype(BF16).astype(F32)
    low_part = gram - high - middle
    ss[...] = jnp.zeros((512, 128), F32)
    ss[pl.ds(3, 64, stride=8), :] = high + pltpu.roll(middle, WIDE, 1)
    ss[pl.ds(7, 64, stride=8), :] = low_part + marks
    alive = alive_ref[...]
    for c in range(3):
        load_ref[64 * c : 64 * c + 64, :] = raw_load_ref[64 * c : 64 * c + 64, :] * alive
        stiff_ref[64 * c : 64 * c + 64, :] = raw_stiff_ref[64 * c : 64 * c + 64, :] * alive
    filled = forces(x_ref, whole_ref, back_ref, map_ref, load_ref, stiff_ref, xs, us)
    out_ref[...] = (filled + ss[...]).astype(BF16)


def apply_maps(map_ref, from_ref, to_ref, dims):
    for b in range(map_ref.shape[0]):
        rows = pl.ds(b, 3, stride=64)
        to_ref[rows, :] = dot(from_ref[rows, :].astype(BF16), map_ref[b], dims)


def forces(x_ref, pick_ref, back_ref, map_ref, load_ref, stiff_ref, xs, us):
    xs[...] = dot(pick_ref[...], x_ref[...])
    apply_maps(map_ref, xs, us, ((1,), (0,)))
    xs[...] = load_ref[...] - stiff_ref[...] * us[...]
    apply_maps(map_ref, xs, us, ((1,), (1,)))
    contrib = jnp.concatenate([us[...].astype(BF16), jnp.zeros((64, 128), BF16)], axis=0)
    return dot(back_ref[...], contrib)


def forces_next_kernel(x_ref, pick_ref, back_ref, map_ref, load_ref, stiff_ref, out_ref, xs, us):
    out_ref[...] = forces(x_ref, pick_ref, back_ref, map_ref, load_ref, stiff_ref, xs, us).astype(BF16)


def final_kernel(x_ref, pick_ref, map_ref, alive_ref, struct_ref, out_ref, disp_ref, xs, us):
    for c in range(3):
        disp_ref[c] = struct_ref[4 * c : 4 * c + 4, :]
    xs[...] = dot(pick_ref[...], x_ref[...])
    apply_maps(map_ref, xs, us, ((1,), (0,)))
    for c in range(3):
        out_ref[64 * c : 64 * c + 64, :] = us[64 * c : 64 * c + 64, :] * alive_ref[...]


def history_sums(hist_ref, vector):
    acc = every(hist_ref, 0) * vector[0:1, :]
    for m in range(1, PARTS):
        acc = acc + every(hist_ref, m) * vector[m : m + 1, :]
    return acc


def as_row(scratch, first, second):
    scratch[...] = jnp.zeros(scratch.shape, F32)
    scratch[0:HIST, :] = first
    if second is not None:
        scratch[WIDE : WIDE + HIST, :] = second
    return dot(jnp.ones((8, 128), F32), scratch[...], ((1,), (1,)), HIGHEST)[0:1, :]


def owner_first_kernel(got_ref, comp_ref, x_ref, hist_ref, msg_ref, image_ref, resid_ref, q_ref, qt_ref, xs, hs):
    got = got_ref[...]
    xs[...] = got.astype(F32)
    mark3 = xs[pl.ds(3, 64, stride=8), :]
    mark7 = xs[pl.ds(7, 64, stride=8), :]
    sum3 = jnp.sum(mark3, axis=0, keepdims=True)
    sum7 = jnp.sum(mark7, axis=0, keepdims=True)
    gram_row = sum3 + pltpu.roll(sum3, WIDE, 1) + pltpu.roll(sum7, WIDE, 1)
    spread = jnp.where(lanes_of((64, 512)) // 8 == rows_of((64, 512)), 1.0, 0.0).astype(BF16)
    wide = dot(mark7.astype(BF16), spread, ((0,), (0,)))
    part = rows_of((16, 512))
    row = lanes_of((16, 512)) % 8
    match = (part // 4 == row % 4) & (part < PARTS)
    q = jnp.where(match & (row < 4), wide[64:80], 0.0)
    q = (q + jnp.where(match & (row >= 4), wide[80:96], 0.0)).astype(BF16)
    q_ref[...] = q
    tall = jnp.broadcast_to(xs[...].reshape(64, 8, 128)[:, 7:8, :], (64, 8, 128)).reshape(512, 128)
    lane = lanes_of((512, 128))
    row = rows_of((512, 128)) % 8
    match = ((lane % 16) // 4 == row % 4) & (lane // 16 - 4 == row // 4) & (lane % 16 < PARTS)
    qt_ref[...] = jnp.where(match, tall, 0.0).astype(BF16)
    image = comp_ref[...] * dot(q, got)[0:PARTS]
    resid = image - x_ref[...]
    image_ref[...] = image
    resid_ref[...] = resid
    line = as_row(hs, history_sums(hist_ref, resid), None)
    line = jnp.where(lanes_of(line.shape) < WIDE, line, gram_row)
    msg_ref[...] = jnp.broadcast_to(line.reshape(1, 1, 128), msg_ref.shape)


def owner_next_kernel(got_ref, q_ref, comp_ref, x_ref, last_ref, hist_ref, msg_ref, image_ref, hs):
    image = comp_ref[...] * dot(q_ref[...], got_ref[...])[0:PARTS]
    image_ref[...] = image
    resid = image - x_ref[...]
    newest = resid - last_ref[...]
    first = rows_of((HIST, 128)) == 0
    own_right = jnp.sum(newest * resid, axis=0, keepdims=True)
    own_row = jnp.sum(newest * newest, axis=0, keepdims=True)
    right = jnp.where(first, own_right, history_sums(hist_ref, resid))
    row = jnp.where(first, own_row, history_sums(hist_ref, newest))
    line = as_row(hs, right, row)
    msg_ref[...] = jnp.broadcast_to(line.reshape(1, 1, 128), msg_ref.shape)


def near_first_kernel(in_ref, out_ref):
    sums = []
    for c in range(2):
        total = in_ref[8 * c]
        for y in range(1, 8):
            total = total + in_ref[8 * c + y]
        sums.append(total)
    right = sums[0] + sums[1]
    rows = jnp.where(lanes_of((1, 128)) < WIDE, pltpu.roll(sums[0], WIDE, 1), sums[1])
    both = jnp.concatenate([right, rows], axis=0)
    out_ref[...] = jnp.broadcast_to(both[None], out_ref.shape)


def near_next_kernel(in_ref, out_ref):
    total = in_ref[0]
    for i in range(1, in_ref.shape[0]):
        total = total + in_ref[i]
    out_ref[...] = jnp.broadcast_to(total[None], out_ref.shape)


def solved(gram, right):
    lanes, rows = lanes_of(gram.shape), rows_of(gram.shape)
    diag = (rows == lanes) & (rows < HIST)
    trace = jnp.sum(jnp.sum(jnp.where(diag, gram, 0.0), axis=1, keepdims=True), axis=0, keepdims=True)
    scale = 1.0 / trace
    a = gram * scale + jnp.where(diag, RIDGE_SHARE / HIST, 0.0)
    a = jnp.where(lanes == WIDE, as_column(right * scale, gram.shape), a)
    tiles = [a[8 * i : 8 * i + 8] for i in range(COLS // 8)]
    sub = rows_of((8, 128))
    for k in range(0, HIST, 2):
        t, s = k // 8, k % 8
        lefts = [jnp.broadcast_to(tile[:, k : k + 1], (8, 128)) for tile in tiles]
        rights = [jnp.broadcast_to(tile[:, k + 1 : k + 2], (8, 128)) for tile in tiles]
        p11, p12 = lefts[t][s : s + 1], rights[t][s : s + 1]
        p21, p22 = lefts[t][s + 1 : s + 2], rights[t][s + 1 : s + 2]
        row1, row2 = tiles[t][s : s + 1], tiles[t][s + 1 : s + 2]
        inverse = 1.0 / (p11 * p22 - p12 * p21)
        new1 = (p22 * row1 - p12 * row2) * inverse
        new2 = (p11 * row2 - p21 * row1) * inverse
        tiles = [tile - left * new1 - right * new2 for tile, left, right in zip(tiles, lefts, rights)]
        tiles[t] = jnp.where(sub == s, new1, jnp.where(sub == s + 1, new2, tiles[t]))
    a = jnp.concatenate(tiles, axis=0)
    return -jnp.broadcast_to(a[:, WIDE : WIDE + 1], a.shape)[:HIST]


def moved(image, coefficients, column):
    lines = [jnp.sum(coefficients * column(m), axis=0, keepdims=True) for m in range(PARTS)]
    return image + jnp.concatenate(lines, axis=0)


def chosen(x, qt, xs):
    xs[...] = jnp.zeros(xs.shape, F32)
    xs[WIDE : WIDE + PARTS, :] = x
    xs[WIDE + 16 : WIDE + 16 + PARTS, :] = x
    return dot(qt, xs[...].astype(BF16)).astype(BF16)


def far_first_kernel(in_ref, image_ref, upd_ref, qt_ref, send_ref, x_ref, gram_ref, hs, gs, xs):
    right = in_ref[0, 0:1, :]
    hs[0:1, :] = in_ref[0, 1:2, :]
    for i in range(1, 32):
        right = right + in_ref[i, 0:1, :]
        hs[i : i + 1, :] = in_ref[i, 1:2, :]
    half = hs[...]
    gs[pl.ds(0, 32, stride=2), :] = half
    gs[pl.ds(1, 32, stride=2), :] = pltpu.roll(half, WIDE, 1)
    gram = gs[0:COLS, :]
    gram = jnp.where(lanes_of(gram.shape) < WIDE, gram, 0.0)
    gram_ref[...] = gram
    coefficients = solved(gram, right)
    x = moved(image_ref[...], coefficients, lambda m: every(upd_ref, m))
    x_ref[...] = x
    send_ref[...] = chosen(x, qt_ref[...], xs)


def far_next_kernel(in_ref, gram_ref, image_ref, last_ref, upd_ref, qt_ref, send_ref, x_ref, xs):
    total = in_ref[0]
    for i in range(1, 32):
        total = total + in_ref[i]
    gram = gram_ref[...]
    lanes, rows = lanes_of(gram.shape), rows_of(gram.shape)
    new_row = jnp.where(lanes_of(total.shape) < WIDE, pltpu.roll(total, WIDE, 1), 0.0)
    gram = jnp.where(rows == 0, new_row, gram)
    gram = jnp.where(lanes == 0, as_column(new_row, gram.shape), gram)
    coefficients = solved(gram, total)
    image = image_ref[...]
    step = image - last_ref[...]
    first = rows_of((HIST, 128)) == 0
    x = moved(image, coefficients, lambda m: jnp.where(first, step[m : m + 1, :], every(upd_ref, m)))
    x_ref[...] = x
    send_ref[...] = chosen(x, qt_ref[...], xs)


def body(
    fluid_load,
    stiffness,
    mapping,
    live_count,
    dest_device,
    local_block,
    compliance,
    start_disp,
    residual_history,
    update_history,
):
    blocks = mapping.shape[0]
    peers = lax.axis_size(FLUID)
    near, far = lax.axis_size(NEAR), lax.axis_size(FAR)
    rows = 8 * peers
    over_fluid = lambda x: exchange(x.reshape(peers, 8, 128), FLUID).reshape(rows, 128)
    parts = lambda a: jnp.swapaxes(a, -3, -2)
    history, updates = (parts(a).reshape(-1, 128) for a in (residual_history, update_history))
    by_part = lambda a: jnp.swapaxes(a, 0, 1).reshape(3 * blocks, 128)
    start = parts(start_disp)[0]
    lines = pltpu.VMEM((3 * blocks, 128), F32)
    square = pltpu.VMEM((128, 128), F32)
    tall = pltpu.VMEM((rows, 128), F32)

    whole, alive = call(
        spread_kernel,
        "spread",
        [((peers, 3, 4, 128), BF16), ((blocks, 128), F32)],
        live_count,
        start,
        in_specs=[SMEM, VMEM],
        cost=pl.CostEstimate(flops=20_000_000_000, bytes_accessed=50_000_000, transcendentals=0),
    )
    whole = exchange(whole, FLUID).reshape(PARTS * peers, 128)
    sent, pick, back, load, stiff, comp, start = call(
        forces_first_kernel,
        "forces_first",
        [
            ((rows, 128), BF16),
            ((3 * blocks, rows), BF16),
            ((rows, 256), BF16),
            ((3 * blocks, 128), F32),
            ((3 * blocks, 128), F32),
            ((PARTS, 128), F32),
            ((PARTS, 128), F32),
        ],
        alive,
        whole,
        dest_device.reshape(1, blocks),
        local_block.reshape(1, blocks),
        history,
        by_part(fluid_load),
        by_part(stiffness),
        mapping,
        parts(compliance)[0],
        start,
        scratch=[
            pltpu.VMEM((64, 128), F32),
            tall,
            pltpu.VMEM((3 * blocks, PARTS * peers), BF16),
            lines,
            lines,
        ],
        mib=8,
    )
    got = over_fluid(sent)
    line, image, resid, q, qt = call(
        owner_first_kernel,
        "owner_first",
        [((near, 1, 128), F32), ((PARTS, 128), F32), ((PARTS, 128), F32), ((16, rows), BF16), ((rows, 128), BF16)],
        got,
        comp,
        start,
        history,
        scratch=[tall, square],
        mib=4,
    )
    line = exchange(line, NEAR)
    line = call(near_first_kernel, "near_first", [((far, 2, 128), F32)], line)[0]
    line = exchange(line, FAR)
    sent, x, gram = call(
        far_first_kernel,
        "far_first",
        [((rows, 128), BF16), ((PARTS, 128), F32), ((COLS, 128), F32)],
        line,
        image,
        updates,
        qt,
        scratch=[pltpu.VMEM((far, 128), F32), pltpu.VMEM((64, 128), F32), square],
    )
    got = over_fluid(sent)
    sent = call(
        forces_next_kernel,
        "forces_next",
        [((rows, 128), BF16)],
        got,
        pick,
        back,
        mapping,
        load,
        stiff,
        scratch=[lines, lines],
        mib=6,
    )[0]
    got = over_fluid(sent)
    last_image = image
    line, image = call(
        owner_next_kernel,
        "owner_next",
        [((near, 1, 128), F32), ((PARTS, 128), F32)],
        got,
        q,
        comp,
        x,
        resid,
        history,
        scratch=[square],
    )
    line = exchange(line, NEAR)
    line = call(near_next_kernel, "near_next", [((far, 1, 128), F32)], line)[0]
    line = exchange(line, FAR)
    sent, struct_disp = call(
        far_next_kernel,
        "far_next",
        [((rows, 128), BF16), ((PARTS, 128), F32)],
        line,
        gram,
        image,
        last_image,
        updates,
        qt,
        scratch=[square],
    )
    got = over_fluid(sent)
    final_disp, struct_disp = call(
        final_kernel,
        "final",
        [((3 * blocks, 128), F32), ((3, 4, 128), F32)],
        got,
        pick,
        mapping,
        alive,
        struct_disp,
        scratch=[lines, lines],
        mib=6,
    )
    struct_disp = parts(struct_disp[None])
    return (struct_disp, jnp.swapaxes(final_disp.reshape(3, blocks, 128), 0, 1))


def solution(mesh):
    split = Mesh(mesh.devices.reshape(8, 4, 2, mesh.shape["solid"]), ALL)
    in_specs = (
        P(ALL, None, None),
        P(ALL, None, None),
        P(ALL, None, None),
        P(ALL),
        P(ALL, None),
        P(ALL),
        P("solid", FLUID, None, None),
        P("solid", FLUID, None, None),
        P(None, "solid", FLUID, None, None),
        P(None, "solid", FLUID, None, None),
    )
    out_specs = (P("solid", FLUID, None, None), P(ALL, None, None))
    return jax.shard_map(body, mesh=split, in_specs=in_specs, out_specs=out_specs, check_vma=False)
```

```python
import jax
import jax.numpy as jnp
from jax import lax
from jax.experimental import pallas as pl
from jax.experimental.pallas import tpu as pltpu
from jax.sharding import Mesh
from jax.sharding import PartitionSpec as P

HIST = 50
RIDGE_SHARE = 0.01
ALL = ("z", "x", "c", "solid")
FLUID = ("z", "x", "c")
NEAR = ("c", "solid")
FAR = ("z", "x")
COLS = 56
PARTS = 12
WIDE = 64
F32, BF16 = jnp.float32, jnp.bfloat16
HIGHEST = lax.Precision.HIGHEST
VMEM = pl.BlockSpec(memory_space=pltpu.VMEM)
SMEM = pl.BlockSpec(memory_space=pltpu.SMEM)


def exchange(x, axes):
    return lax.all_to_all(x, axes, split_axis=0, concat_axis=0, tiled=True)


def call(kernel, name, outs, *args, in_specs=None, scratch=(), mib=2, cost=None):
    return pl.pallas_call(
        kernel,
        out_shape=[jax.ShapeDtypeStruct(shape, dtype) for shape, dtype in outs],
        compiler_params=pltpu.CompilerParams(vmem_limit_bytes=mib << 20),
        in_specs=in_specs or [VMEM] * len(args),
        out_specs=[VMEM] * len(outs),
        scratch_shapes=list(scratch),
        cost_estimate=cost,
        name=name,
    )(*args)


def dot(a, b, dims=((1,), (0,)), precision=None):
    return lax.dot_general(a, b, (dims, ((), ())), precision=precision, preferred_element_type=F32)


def lanes_of(shape):
    return lax.broadcasted_iota(jnp.int32, shape, len(shape) - 1)


def rows_of(shape):
    return lax.broadcasted_iota(jnp.int32, shape, 0)


def every(ref, part):
    return ref[pl.ds(part, HIST, stride=PARTS), :]


def as_column(row, shape):
    on_diag = lanes_of(shape) == rows_of(shape)
    return jnp.sum(jnp.where(on_diag, row, jnp.zeros_like(row)), axis=1, keepdims=True)


def sixths(i):
    peer = jnp.floor((i.astype(F32) + 0.5) * (1.0 / 6.0)).astype(jnp.int32)
    row = i - 6 * peer
    return peer, row // 2, row % 2


def spread_kernel(live_ref, x_ref, out_ref, alive_ref):
    out_ref[...] = jnp.broadcast_to(x_ref[...].astype(BF16)[None], out_ref.shape)
    alive_ref[...] = jnp.where(rows_of(alive_ref.shape) < live_ref[0], 1.0, 0.0)


def forces_first_kernel(
    alive_ref, x_ref, dest_ref, local_ref, hist_ref, raw_load_ref, raw_stiff_ref, map_ref, comp_ref, start_ref,
    out_ref, pick_ref, back_ref, load_ref, stiff_ref, flat_comp_ref, flat_start_ref, gs, ss, whole_ref, back_first_ref, xs, us,
):
    for c in range(3):
        flat_comp_ref[4 * c : 4 * c + 4, :] = comp_ref[c]
        flat_start_ref[4 * c : 4 * c + 4, :] = start_ref[c]
    square = (64, 128)
    lanes, rows = lanes_of(square), rows_of(square)
    dest = jnp.where(lanes < 64, jnp.concatenate([dest_ref[...]] * 2, axis=1), -1)
    local = jnp.concatenate([local_ref[...]] * 2, axis=1)
    dest_column = as_column(dest.astype(F32), square)
    local_column = as_column(local.astype(F32), square).astype(jnp.int32)
    same = (dest_column == dest.astype(F32)) & (lanes < 64)
    dest_column = dest_column.astype(jnp.int32)
    slot_column = jnp.sum(jnp.where(same & (lanes < rows), 1.0, 0.0), axis=1, keepdims=True)
    slot_row = jnp.sum(jnp.where(same & (rows < lanes), 1.0, 0.0), axis=0, keepdims=True)
    slot_column = slot_column.astype(jnp.int32)
    place_row = dest[0:1] * 8 + slot_row.astype(jnp.int32) * 4
    wide = lanes_of((64, 384))
    wider = lanes_of((64, 768))
    for c in range(3):
        pick_ref[64 * c : 64 * c + 64, :] = jnp.where(wide == dest_column * 6 + 2 * c + slot_column, 1.0, 0.0).astype(BF16)
        whole_column = dest_column * PARTS + 4 * c + local_column
        whole_ref[64 * c : 64 * c + 64, :] = jnp.where(wider == whole_column, 1.0, 0.0).astype(BF16)
    low = lanes[0:1] < 64
    place_next = dest[0:1] * 6 + slot_row.astype(jnp.int32)
    for place, step, ref in ((place_row, 1, back_first_ref), (place_next, 2, back_ref)):
        tall = rows_of((ref.shape[0], 128))
        first = jnp.where(low, place, pltpu.roll(place, 64, 1) + step)
        second = jnp.where(low, place + 2 * step, -1)
        ref[:, 0:128] = jnp.where(tall == first, 1.0, 0.0).astype(BF16)
        ref[:, 128:256] = jnp.where(tall == second, 1.0, 0.0).astype(BF16)
    part = lanes % 16
    held = (lanes >= 64) & (lanes // 16 - 4 == slot_column) & (part % 4 == local_column) & (part < PARTS)
    onto = jnp.where(dest == rows, 1.0, 0.0).astype(BF16)
    marks = dot(onto[:, 0:64], jnp.where(held, 1.0, 0.0).astype(BF16))
    history = jnp.concatenate([every(hist_ref, m) for m in range(PARTS)], axis=1)
    gs[...] = jnp.zeros(square, F32)
    gs[0:HIST, 0:HIST] = dot(history, history, ((1,), (1,)), HIGHEST)
    gram = gs[...]
    high = gram.astype(BF16).astype(F32)
    middle = (gram - high).astype(BF16).astype(F32)
    low_part = gram - high - middle
    ss[...] = jnp.zeros((512, 128), F32)
    ss[pl.ds(3, 64, stride=8), :] = high + pltpu.roll(middle, WIDE, 1)
    ss[pl.ds(7, 64, stride=8), :] = low_part + marks
    alive = alive_ref[...]
    for c in range(3):
        load_ref[64 * c : 64 * c + 64, :] = raw_load_ref[64 * c : 64 * c + 64, :] * alive
        stiff_ref[64 * c : 64 * c + 64, :] = raw_stiff_ref[64 * c : 64 * c + 64, :] * alive
    filled = forces(x_ref, whole_ref, back_first_ref, map_ref, load_ref, stiff_ref, xs, us)
    out_ref[...] = (filled + ss[...]).astype(BF16)


def apply_maps(map_ref, from_ref, to_ref, dims):
    for b in range(map_ref.shape[0]):
        rows = pl.ds(b, 3, stride=64)
        to_ref[rows, :] = dot(from_ref[rows, :].astype(BF16), map_ref[b], dims)


def forces(x_ref, pick_ref, back_ref, map_ref, load_ref, stiff_ref, xs, us):
    xs[...] = dot(pick_ref[...], x_ref[...])
    apply_maps(map_ref, xs, us, ((1,), (0,)))
    xs[...] = load_ref[...] - stiff_ref[...] * us[...]
    apply_maps(map_ref, xs, us, ((1,), (1,)))
    contrib = jnp.concatenate([us[...].astype(BF16), jnp.zeros((64, 128), BF16)], axis=0)
    return dot(back_ref[...], contrib)


def forces_next_kernel(x_ref, pick_ref, back_ref, map_ref, load_ref, stiff_ref, out_ref, xs, us):
    out_ref[...] = forces(x_ref, pick_ref, back_ref, map_ref, load_ref, stiff_ref, xs, us).astype(BF16)


def final_kernel(x_ref, pick_ref, map_ref, alive_ref, struct_ref, out_ref, disp_ref, xs, us):
    disp_ref[...] = struct_ref[...]
    xs[...] = dot(pick_ref[...], x_ref[...])
    apply_maps(map_ref, xs, us, ((1,), (0,)))
    for c in range(3):
        out_ref[64 * c : 64 * c + 64, :] = us[64 * c : 64 * c + 64, :] * alive_ref[...]


def history_sums(hist_ref, vector):
    acc = every(hist_ref, 0) * vector[0:1, :]
    for m in range(1, PARTS):
        acc = acc + every(hist_ref, m) * vector[m : m + 1, :]
    return acc


def as_row(scratch, first, second):
    scratch[...] = jnp.zeros(scratch.shape, F32)
    scratch[0:HIST, :] = first
    if second is not None:
        scratch[WIDE : WIDE + HIST, :] = second
    return dot(jnp.ones((8, 128), F32), scratch[...], ((1,), (1,)), HIGHEST)[0:1, :]


def owner_first_kernel(got_ref, comp_ref, x_ref, hist_ref, msg_ref, image_ref, resid_ref, q_ref, qt_ref, xs, hs):
    got = got_ref[...]
    xs[...] = got.astype(F32)
    mark3 = xs[pl.ds(3, 64, stride=8), :]
    mark7 = xs[pl.ds(7, 64, stride=8), :]
    sum3 = jnp.sum(mark3, axis=0, keepdims=True)
    sum7 = jnp.sum(mark7, axis=0, keepdims=True)
    gram_row = sum3 + pltpu.roll(sum3, WIDE, 1) + pltpu.roll(sum7, WIDE, 1)
    spread = jnp.where(lanes_of((64, 512)) // 8 == rows_of((64, 512)), 1.0, 0.0).astype(BF16)
    wide = dot(mark7.astype(BF16), spread, ((0,), (0,)))
    part = rows_of((16, 512))
    row = lanes_of((16, 512)) % 8
    match = (part // 4 == row % 4) & (part < PARTS)
    q = jnp.where(match & (row < 4), wide[64:80], 0.0)
    q = (q + jnp.where(match & (row >= 4), wide[80:96], 0.0)).astype(BF16)
    peer, component, place = sixths(lanes_of((64, 384)))
    spread = jnp.where(peer == rows_of((64, 384)), 1.0, 0.0).astype(BF16)
    wide = dot(mark7.astype(BF16), spread, ((0,), (0,)))
    part = rows_of((16, 384))
    match = (part // 4 == component[0:16]) & (part < PARTS)
    later = jnp.where(match & (place[0:16] == 0), wide[64:80], 0.0)
    q_ref[...] = (later + jnp.where(match & (place[0:16] == 1), wide[80:96], 0.0)).astype(BF16)
    peer, component, place = sixths(rows_of((384, 128)))
    lane = lanes_of((384, 128))
    spread = jnp.where(peer == lane, 1.0, 0.0).astype(BF16)
    tall = dot(spread[:, 0:64], mark7.astype(BF16))
    match = ((lane % 16) // 4 == component) & (lane // 16 - 4 == place) & (lane % 16 < PARTS)
    qt_ref[...] = jnp.where(match, tall, 0.0).astype(BF16)
    image = comp_ref[...] * dot(q, got)[0:PARTS]
    resid = image - x_ref[...]
    image_ref[...] = image
    resid_ref[...] = resid
    line = as_row(hs, history_sums(hist_ref, resid), None)
    line = jnp.where(lanes_of(line.shape) < WIDE, line, gram_row)
    msg_ref[...] = jnp.broadcast_to(line.reshape(1, 1, 128), msg_ref.shape)


def owner_next_kernel(got_ref, q_ref, comp_ref, x_ref, last_ref, hist_ref, msg_ref, image_ref, hs):
    image = comp_ref[...] * dot(q_ref[...], got_ref[...])[0:PARTS]
    image_ref[...] = image
    resid = image - x_ref[...]
    newest = resid - last_ref[...]
    first = rows_of((HIST, 128)) == 0
    own_right = jnp.sum(newest * resid, axis=0, keepdims=True)
    own_row = jnp.sum(newest * newest, axis=0, keepdims=True)
    right = jnp.where(first, own_right, history_sums(hist_ref, resid))
    row = jnp.where(first, own_row, history_sums(hist_ref, newest))
    line = as_row(hs, right, row)
    msg_ref[...] = jnp.broadcast_to(line.reshape(1, 1, 128), msg_ref.shape)


def near_first_kernel(in_ref, out_ref):
    sums = []
    for c in range(2):
        total = in_ref[8 * c]
        for y in range(1, 8):
            total = total + in_ref[8 * c + y]
        sums.append(total)
    right = sums[0] + sums[1]
    rows = jnp.where(lanes_of((1, 128)) < WIDE, pltpu.roll(sums[0], WIDE, 1), sums[1])
    both = jnp.concatenate([right, rows], axis=0)
    out_ref[...] = jnp.broadcast_to(both[None], out_ref.shape)


def near_next_kernel(in_ref, out_ref):
    total = in_ref[0]
    for i in range(1, in_ref.shape[0]):
        total = total + in_ref[i]
    out_ref[...] = jnp.broadcast_to(total[None], out_ref.shape)


def solved(gram, right):
    lanes, rows = lanes_of(gram.shape), rows_of(gram.shape)
    diag = (rows == lanes) & (rows < HIST)
    trace = jnp.sum(jnp.sum(jnp.where(diag, gram, 0.0), axis=1, keepdims=True), axis=0, keepdims=True)
    scale = 1.0 / trace
    a = gram * scale + jnp.where(diag, RIDGE_SHARE / HIST, 0.0)
    a = jnp.where(lanes == WIDE, as_column(right * scale, gram.shape), a)
    tiles = [a[8 * i : 8 * i + 8] for i in range(COLS // 8)]
    sub = rows_of((8, 128))
    column = lambda k: [jnp.broadcast_to(tile[:, k : k + 1], (8, 128)) for tile in tiles]
    at = lambda stack, k: stack[k // 8][k % 8 : k % 8 + 1]
    lefts, rights = column(0), column(1)
    for k in range(0, HIST, 2):
        coming = [(j, column(j)) for j in (k + 2, k + 3) if j < HIST]
        p11, p12, p21, p22 = at(lefts, k), at(rights, k), at(lefts, k + 1), at(rights, k + 1)
        inverse = 1.0 / (p11 * p22 - p12 * p21)

        def scaled(one, two):
            return (p22 * one - p12 * two) * inverse, (p11 * two - p21 * one) * inverse

        def reduced(stack, new1, new2):
            out = [v - left * new1 - right * new2 for v, left, right in zip(stack, lefts, rights)]
            t, r = k // 8, k % 8
            out[t] = jnp.where(sub == r, new1, jnp.where(sub == r + 1, new2, out[t]))
            return out

        following = [reduced(old, *scaled(at(lefts, j), at(rights, j))) for j, old in coming]
        tiles = reduced(tiles, *scaled(at(tiles, k), at(tiles, k + 1)))
        if following:
            lefts, rights = following
    a = jnp.concatenate(tiles, axis=0)
    return -jnp.broadcast_to(a[:, WIDE : WIDE + 1], a.shape)[:HIST]


def moved(image, coefficients, column):
    lines = [jnp.sum(coefficients * column(m), axis=0, keepdims=True) for m in range(PARTS)]
    return image + jnp.concatenate(lines, axis=0)


def chosen(x, qt, xs):
    xs[...] = jnp.zeros(xs.shape, F32)
    xs[WIDE : WIDE + PARTS, :] = x
    xs[WIDE + 16 : WIDE + 16 + PARTS, :] = x
    return dot(qt, xs[...].astype(BF16)).astype(BF16)


def far_first_kernel(in_ref, image_ref, upd_ref, qt_ref, send_ref, x_ref, gram_ref, hs, gs, xs):
    right = in_ref[0, 0:1, :]
    hs[0:1, :] = in_ref[0, 1:2, :]
    for i in range(1, 32):
        right = right + in_ref[i, 0:1, :]
        hs[i : i + 1, :] = in_ref[i, 1:2, :]
    half = hs[...]
    gs[pl.ds(0, 32, stride=2), :] = half
    gs[pl.ds(1, 32, stride=2), :] = pltpu.roll(half, WIDE, 1)
    gram = gs[0:COLS, :]
    gram = jnp.where(lanes_of(gram.shape) < WIDE, gram, 0.0)
    gram_ref[...] = gram
    coefficients = solved(gram, right)
    x = moved(image_ref[...], coefficients, lambda m: every(upd_ref, m))
    x_ref[...] = x
    send_ref[...] = chosen(x, qt_ref[...], xs)


def far_next_kernel(in_ref, gram_ref, image_ref, last_ref, upd_ref, qt_ref, send_ref, x_ref, xs):
    total = in_ref[0]
    for i in range(1, 32):
        total = total + in_ref[i]
    gram = gram_ref[...]
    lanes, rows = lanes_of(gram.shape), rows_of(gram.shape)
    new_row = jnp.where(lanes_of(total.shape) < WIDE, pltpu.roll(total, WIDE, 1), 0.0)
    gram = jnp.where(rows == 0, new_row, gram)
    gram = jnp.where(lanes == 0, as_column(new_row, gram.shape), gram)
    coefficients = solved(gram, total)
    image = image_ref[...]
    step = image - last_ref[...]
    first = rows_of((HIST, 128)) == 0
    x = moved(image, coefficients, lambda m: jnp.where(first, step[m : m + 1, :], every(upd_ref, m)))
    for c in range(3):
        x_ref[c] = x[4 * c : 4 * c + 4, :]
    send_ref[...] = chosen(x, qt_ref[...], xs)


def body(
    fluid_load,
    stiffness,
    mapping,
    live_count,
    dest_device,
    local_block,
    compliance,
    start_disp,
    residual_history,
    update_history,
):
    blocks = mapping.shape[0]
    peers = lax.axis_size(FLUID)
    near, far = lax.axis_size(NEAR), lax.axis_size(FAR)
    rows = 8 * peers
    later = 6 * peers
    over_fluid = lambda x: exchange(x.reshape(peers, 3, 2, 128), FLUID).reshape(later, 128)
    parts = lambda a: jnp.swapaxes(a, -3, -2)
    history, updates = (parts(a).reshape(-1, 128) for a in (residual_history, update_history))
    by_part = lambda a: jnp.swapaxes(a, 0, 1).reshape(3 * blocks, 128)
    start = parts(start_disp)[0]
    lines = pltpu.VMEM((3 * blocks, 128), F32)
    square = pltpu.VMEM((128, 128), F32)
    tall = pltpu.VMEM((rows, 128), F32)

    whole, alive = call(
        spread_kernel,
        "spread",
        [((peers, 3, 4, 128), BF16), ((blocks, 128), F32)],
        live_count,
        start,
        in_specs=[SMEM, VMEM],
        cost=pl.CostEstimate(flops=20_000_000_000, bytes_accessed=50_000_000, transcendentals=0),
    )
    whole = exchange(whole, FLUID).reshape(PARTS * peers, 128)
    sent, pick, back, load, stiff, comp, start = call(
        forces_first_kernel,
        "forces_first",
        [
            ((rows, 128), BF16),
            ((3 * blocks, later), BF16),
            ((later, 256), BF16),
            ((3 * blocks, 128), F32),
            ((3 * blocks, 128), F32),
            ((PARTS, 128), F32),
            ((PARTS, 128), F32),
        ],
        alive,
        whole,
        dest_device.reshape(1, blocks),
        local_block.reshape(1, blocks),
        history,
        by_part(fluid_load),
        by_part(stiffness),
        mapping,
        parts(compliance)[0],
        start,
        scratch=[
            pltpu.VMEM((64, 128), F32),
            tall,
            pltpu.VMEM((3 * blocks, PARTS * peers), BF16),
            pltpu.VMEM((rows, 256), BF16),
            lines,
            lines,
        ],
        mib=8,
    )
    got = exchange(sent.reshape(peers, 8, 128), FLUID).reshape(rows, 128)
    line, image, resid, q, qt = call(
        owner_first_kernel,
        "owner_first",
        [((near, 1, 128), F32), ((PARTS, 128), F32), ((PARTS, 128), F32), ((16, later), BF16), ((later, 128), BF16)],
        got,
        comp,
        start,
        history,
        scratch=[tall, square],
        mib=4,
    )
    line = exchange(line, NEAR)
    line = call(near_first_kernel, "near_first", [((far, 2, 128), F32)], line)[0]
    line = exchange(line, FAR)
    sent, x, gram = call(
        far_first_kernel,
        "far_first",
        [((later, 128), BF16), ((PARTS, 128), F32), ((COLS, 128), F32)],
        line,
        image,
        updates,
        qt,
        scratch=[pltpu.VMEM((far, 128), F32), pltpu.VMEM((64, 128), F32), square],
    )
    got = over_fluid(sent)
    sent = call(
        forces_next_kernel,
        "forces_next",
        [((later, 128), BF16)],
        got,
        pick,
        back,
        mapping,
        load,
        stiff,
        scratch=[lines, lines],
        mib=6,
    )[0]
    got = over_fluid(sent)
    last_image = image
    line, image = call(
        owner_next_kernel,
        "owner_next",
        [((near, 1, 128), F32), ((PARTS, 128), F32)],
        got,
        q,
        comp,
        x,
        resid,
        history,
        scratch=[square],
    )
    line = exchange(line, NEAR)
    line = call(near_next_kernel, "near_next", [((far, 1, 128), F32)], line)[0]
    line = exchange(line, FAR)
    sent, struct_disp = call(
        far_next_kernel,
        "far_next",
        [((later, 128), BF16), ((3, 4, 128), F32)],
        line,
        gram,
        image,
        last_image,
        updates,
        qt,
        scratch=[square],
    )
    got = over_fluid(sent)
    final_disp, struct_disp = call(
        final_kernel,
        "final",
        [((3 * blocks, 128), F32), ((3, 4, 128), F32)],
        got,
        pick,
        mapping,
        alive,
        struct_disp,
        scratch=[lines, lines],
        mib=6,
    )
    struct_disp = parts(struct_disp[None])
    return (struct_disp, jnp.swapaxes(final_disp.reshape(3, blocks, 128), 0, 1))


def solution(mesh):
    split = Mesh(mesh.devices.reshape(8, 4, 2, mesh.shape["solid"]), ALL)
    in_specs = (
        P(ALL, None, None),
        P(ALL, None, None),
        P(ALL, None, None),
        P(ALL),
        P(ALL, None),
        P(ALL),
        P("solid", FLUID, None, None),
        P("solid", FLUID, None, None),
        P(None, "solid", FLUID, None, None),
        P(None, "solid", FLUID, None, None),
    )
    out_specs = (P("solid", FLUID, None, None), P(ALL, None, None))
    return jax.shard_map(body, mesh=split, in_specs=in_specs, out_specs=out_specs, check_vma=False)
```

```python
import jax
import jax.numpy as jnp
from jax import lax
from jax.experimental import pallas as pl
from jax.experimental.pallas import tpu as pltpu
from jax.sharding import Mesh
from jax.sharding import PartitionSpec as P

HIST = 50
RIDGE_SHARE = 0.01
ALL = ("z", "x", "c", "solid")
FLUID = ("z", "x", "c")
NEAR = ("c", "solid")
FAR = ("z", "x")
COLS = 56
PARTS = 12
WIDE = 64
F32, BF16 = jnp.float32, jnp.bfloat16
HIGHEST = lax.Precision.HIGHEST
VMEM = pl.BlockSpec(memory_space=pltpu.VMEM)
SMEM = pl.BlockSpec(memory_space=pltpu.SMEM)


def exchange(x, axes):
    return lax.all_to_all(x, axes, split_axis=0, concat_axis=0, tiled=True)


def call(kernel, name, outs, *args, in_specs=None, scratch=(), mib=2, cost=None):
    return pl.pallas_call(
        kernel,
        out_shape=[jax.ShapeDtypeStruct(shape, dtype) for shape, dtype in outs],
        compiler_params=pltpu.CompilerParams(vmem_limit_bytes=mib << 20),
        in_specs=in_specs or [VMEM] * len(args),
        out_specs=[VMEM] * len(outs),
        scratch_shapes=list(scratch),
        cost_estimate=cost,
        name=name,
    )(*args)


def dot(a, b, dims=((1,), (0,)), precision=None):
    return lax.dot_general(a, b, (dims, ((), ())), precision=precision, preferred_element_type=F32)


def lanes_of(shape):
    return lax.broadcasted_iota(jnp.int32, shape, len(shape) - 1)


def rows_of(shape):
    return lax.broadcasted_iota(jnp.int32, shape, 0)


def every(ref, part):
    return ref[pl.ds(part, HIST, stride=PARTS), :]


def as_column(row, shape):
    on_diag = lanes_of(shape) == rows_of(shape)
    return jnp.sum(jnp.where(on_diag, row, jnp.zeros_like(row)), axis=1, keepdims=True)


def sixths(i):
    peer = jnp.floor((i.astype(F32) + 0.5) * (1.0 / 6.0)).astype(jnp.int32)
    row = i - 6 * peer
    return peer, row // 2, row % 2


def spread_kernel(live_ref, x_ref, out_ref, alive_ref):
    out_ref[...] = jnp.broadcast_to(x_ref[...].astype(BF16)[None], out_ref.shape)
    alive_ref[...] = jnp.where(rows_of(alive_ref.shape) < live_ref[0], 1.0, 0.0)


def forces_first_kernel(
    alive_ref, x_ref, dest_ref, local_ref, hist_ref, raw_load_ref, raw_stiff_ref, map_ref, comp_ref, start_ref,
    out_ref, pick_ref, back_ref, load_ref, stiff_ref, flat_comp_ref, flat_start_ref, gs, ss, whole_ref, back_first_ref, xs, us,
):
    for c in range(3):
        flat_comp_ref[4 * c : 4 * c + 4, :] = comp_ref[c]
        flat_start_ref[4 * c : 4 * c + 4, :] = start_ref[c]
    square = (64, 128)
    lanes, rows = lanes_of(square), rows_of(square)
    dest = jnp.where(lanes < 64, jnp.concatenate([dest_ref[...]] * 2, axis=1), -1)
    local = jnp.concatenate([local_ref[...]] * 2, axis=1)
    dest_column = as_column(dest.astype(F32), square)
    local_column = as_column(local.astype(F32), square).astype(jnp.int32)
    same = (dest_column == dest.astype(F32)) & (lanes < 64)
    dest_column = dest_column.astype(jnp.int32)
    slot_column = jnp.sum(jnp.where(same & (lanes < rows), 1.0, 0.0), axis=1, keepdims=True)
    slot_row = jnp.sum(jnp.where(same & (rows < lanes), 1.0, 0.0), axis=0, keepdims=True)
    slot_column = slot_column.astype(jnp.int32)
    place_row = dest[0:1] * 8 + slot_row.astype(jnp.int32) * 4
    wide = lanes_of((64, 384))
    wider = lanes_of((64, 768))
    for c in range(3):
        pick_ref[64 * c : 64 * c + 64, :] = jnp.where(wide == dest_column * 6 + 2 * c + slot_column, 1.0, 0.0).astype(BF16)
        whole_column = dest_column * PARTS + 4 * c + local_column
        whole_ref[64 * c : 64 * c + 64, :] = jnp.where(wider == whole_column, 1.0, 0.0).astype(BF16)
    low = lanes[0:1] < 64
    place_next = dest[0:1] * 6 + slot_row.astype(jnp.int32)
    for place, step, ref in ((place_row, 1, back_first_ref), (place_next, 2, back_ref)):
        tall = rows_of((ref.shape[0], 128))
        first = jnp.where(low, place, pltpu.roll(place, 64, 1) + step)
        second = jnp.where(low, place + 2 * step, -1)
        ref[:, 0:128] = jnp.where(tall == first, 1.0, 0.0).astype(BF16)
        ref[:, 128:256] = jnp.where(tall == second, 1.0, 0.0).astype(BF16)
    part = lanes % 16
    held = (lanes >= 64) & (lanes // 16 - 4 == slot_column) & (part % 4 == local_column) & (part < PARTS)
    onto = jnp.where(dest == rows, 1.0, 0.0).astype(BF16)
    marks = dot(onto[:, 0:64], jnp.where(held, 1.0, 0.0).astype(BF16))
    history = jnp.concatenate([every(hist_ref, m) for m in range(PARTS)], axis=1)
    gs[...] = jnp.zeros(square, F32)
    gs[0:HIST, 0:HIST] = dot(history, history, ((1,), (1,)), HIGHEST)
    gram = gs[...]
    high = gram.astype(BF16).astype(F32)
    middle = (gram - high).astype(BF16).astype(F32)
    low_part = gram - high - middle
    ss[...] = jnp.zeros((512, 128), F32)
    ss[pl.ds(3, 64, stride=8), :] = high + pltpu.roll(middle, WIDE, 1)
    ss[pl.ds(7, 64, stride=8), :] = low_part + marks
    alive = alive_ref[...]
    for c in range(3):
        load_ref[64 * c : 64 * c + 64, :] = raw_load_ref[64 * c : 64 * c + 64, :] * alive
        stiff_ref[64 * c : 64 * c + 64, :] = raw_stiff_ref[64 * c : 64 * c + 64, :] * alive
    filled = forces(x_ref, whole_ref, back_first_ref, map_ref, load_ref, stiff_ref, xs, us)
    out_ref[...] = (filled + ss[...]).astype(BF16)


def apply_maps(map_ref, from_ref, to_ref, dims):
    for b in range(0, map_ref.shape[0], 2):
        first, second = pl.ds(b, 3, stride=64), pl.ds(b + 1, 3, stride=64)
        both = jnp.concatenate([from_ref[first, :], from_ref[second, :]], axis=0).astype(BF16)
        if dims == ((1,), (0,)):
            maps = jnp.concatenate([map_ref[b], map_ref[b + 1]], axis=1)
        else:
            maps = map_ref[b : b + 2].reshape(256, 128)
        out = dot(both, maps, dims)
        to_ref[first, :] = out[0:3, 0:128]
        to_ref[second, :] = out[3:6, 128:256]


def forces(x_ref, pick_ref, back_ref, map_ref, load_ref, stiff_ref, xs, us):
    xs[...] = dot(pick_ref[...], x_ref[...])
    apply_maps(map_ref, xs, us, ((1,), (0,)))
    xs[...] = load_ref[...] - stiff_ref[...] * us[...]
    apply_maps(map_ref, xs, us, ((1,), (1,)))
    contrib = jnp.concatenate([us[...].astype(BF16), jnp.zeros((64, 128), BF16)], axis=0)
    return dot(back_ref[...], contrib)


def forces_next_kernel(x_ref, pick_ref, back_ref, map_ref, load_ref, stiff_ref, out_ref, xs, us):
    out_ref[...] = forces(x_ref, pick_ref, back_ref, map_ref, load_ref, stiff_ref, xs, us).astype(BF16)


def final_kernel(x_ref, pick_ref, map_ref, alive_ref, struct_ref, out_ref, disp_ref, xs, us):
    disp_ref[...] = struct_ref[...]
    xs[...] = dot(pick_ref[...], x_ref[...])
    apply_maps(map_ref, xs, us, ((1,), (0,)))
    for c in range(3):
        out_ref[64 * c : 64 * c + 64, :] = us[64 * c : 64 * c + 64, :] * alive_ref[...]


def history_sums(hist_ref, vector):
    acc = every(hist_ref, 0) * vector[0:1, :]
    for m in range(1, PARTS):
        acc = acc + every(hist_ref, m) * vector[m : m + 1, :]
    return acc


def as_row(scratch, first, second):
    scratch[...] = jnp.zeros(scratch.shape, F32)
    scratch[0:HIST, :] = first
    if second is not None:
        scratch[WIDE : WIDE + HIST, :] = second
    return dot(jnp.ones((8, 128), F32), scratch[...], ((1,), (1,)), HIGHEST)[0:1, :]


def owner_first_kernel(got_ref, comp_ref, x_ref, hist_ref, msg_ref, image_ref, resid_ref, q_ref, qt_ref, xs, hs):
    got = got_ref[...]
    xs[...] = got.astype(F32)
    mark3 = xs[pl.ds(3, 64, stride=8), :]
    mark7 = xs[pl.ds(7, 64, stride=8), :]
    sum3 = jnp.sum(mark3, axis=0, keepdims=True)
    sum7 = jnp.sum(mark7, axis=0, keepdims=True)
    gram_row = sum3 + pltpu.roll(sum3, WIDE, 1) + pltpu.roll(sum7, WIDE, 1)
    spread = jnp.where(lanes_of((64, 512)) // 8 == rows_of((64, 512)), 1.0, 0.0).astype(BF16)
    wide = dot(mark7.astype(BF16), spread, ((0,), (0,)))
    part = rows_of((16, 512))
    row = lanes_of((16, 512)) % 8
    match = (part // 4 == row % 4) & (part < PARTS)
    q = jnp.where(match & (row < 4), wide[64:80], 0.0)
    q = (q + jnp.where(match & (row >= 4), wide[80:96], 0.0)).astype(BF16)
    peer, component, place = sixths(lanes_of((64, 384)))
    spread = jnp.where(peer == rows_of((64, 384)), 1.0, 0.0).astype(BF16)
    wide = dot(mark7.astype(BF16), spread, ((0,), (0,)))
    part = rows_of((16, 384))
    match = (part // 4 == component[0:16]) & (part < PARTS)
    later = jnp.where(match & (place[0:16] == 0), wide[64:80], 0.0)
    q_ref[...] = (later + jnp.where(match & (place[0:16] == 1), wide[80:96], 0.0)).astype(BF16)
    peer, component, place = sixths(rows_of((384, 128)))
    lane = lanes_of((384, 128))
    spread = jnp.where(peer == lane, 1.0, 0.0).astype(BF16)
    tall = dot(spread[:, 0:64], mark7.astype(BF16))
    match = ((lane % 16) // 4 == component) & (lane // 16 - 4 == place) & (lane % 16 < PARTS)
    qt_ref[...] = jnp.where(match, tall, 0.0).astype(BF16)
    image = comp_ref[...] * dot(q, got)[0:PARTS]
    resid = image - x_ref[...]
    image_ref[...] = image
    resid_ref[...] = resid
    line = as_row(hs, history_sums(hist_ref, resid), None)
    line = jnp.where(lanes_of(line.shape) < WIDE, line, gram_row)
    msg_ref[...] = jnp.broadcast_to(line.reshape(1, 1, 128), msg_ref.shape)


def owner_next_kernel(got_ref, q_ref, comp_ref, x_ref, last_ref, hist_ref, msg_ref, image_ref, hs):
    image = comp_ref[...] * dot(q_ref[...], got_ref[...])[0:PARTS]
    image_ref[...] = image
    resid = image - x_ref[...]
    newest = resid - last_ref[...]
    first = rows_of((HIST, 128)) == 0
    own_right = jnp.sum(newest * resid, axis=0, keepdims=True)
    own_row = jnp.sum(newest * newest, axis=0, keepdims=True)
    right = jnp.where(first, own_right, history_sums(hist_ref, resid))
    row = jnp.where(first, own_row, history_sums(hist_ref, newest))
    line = as_row(hs, right, row)
    msg_ref[...] = jnp.broadcast_to(line.reshape(1, 1, 128), msg_ref.shape)


def near_first_kernel(in_ref, out_ref):
    sums = []
    for c in range(2):
        total = in_ref[8 * c]
        for y in range(1, 8):
            total = total + in_ref[8 * c + y]
        sums.append(total)
    right = sums[0] + sums[1]
    rows = jnp.where(lanes_of((1, 128)) < WIDE, pltpu.roll(sums[0], WIDE, 1), sums[1])
    both = jnp.concatenate([right, rows], axis=0)
    out_ref[...] = jnp.broadcast_to(both[None], out_ref.shape)


def near_next_kernel(in_ref, out_ref):
    total = in_ref[0]
    for i in range(1, in_ref.shape[0]):
        total = total + in_ref[i]
    out_ref[...] = jnp.broadcast_to(total[None], out_ref.shape)


def solved(gram, right):
    lanes, rows = lanes_of(gram.shape), rows_of(gram.shape)
    diag = (rows == lanes) & (rows < HIST)
    trace = jnp.sum(jnp.sum(jnp.where(diag, gram, 0.0), axis=1, keepdims=True), axis=0, keepdims=True)
    scale = 1.0 / trace
    a = gram * scale + jnp.where(diag, RIDGE_SHARE / HIST, 0.0)
    a = jnp.where(lanes == rows + WIDE, 1.0, a)
    under = jnp.where(lanes_of(right.shape) < WIDE, right * scale, 0.0)
    tiles = [a[8 * i : 8 * i + 8] for i in range(COLS // 8)] + [jnp.broadcast_to(under, (8, 128))]
    spread = lambda k, start: [jnp.broadcast_to(tile[:, k : k + 1], (8, 128)) for tile in tiles[start:]]
    lefts, rights = spread(0, 0), spread(1, 0)
    for k in range(0, HIST, 2):
        first = k // 8
        at = lambda stack, j: stack[j // 8 - first][j % 8 : j % 8 + 1]
        coming = [(j, spread(j, first)) for j in (k + 2, k + 3) if j < HIST]
        p11, p12, p21, p22 = at(lefts, k), at(rights, k), at(lefts, k + 1), at(rights, k + 1)
        inverse = 1.0 / (p11 * p22 - p12 * p21)

        def scaled(one, two):
            return (p22 * one - p12 * two) * inverse, (p11 * two - p21 * one) * inverse

        def reduced(stack, new1, new2):
            return [v - left * new1 - right * new2 for v, left, right in zip(stack, lefts, rights)]

        following = [reduced(old, *scaled(at(lefts, j), at(rights, j))) for j, old in coming]
        tiles[first:] = reduced(tiles[first:], *scaled(at(tiles[first:], k), at(tiles[first:], k + 1)))
        if following:
            lefts, rights = (stack[(k + 2) // 8 - first :] for stack in following)
    solution_row = pltpu.roll(tiles[-1], WIDE, 1)[0:1]
    return jnp.broadcast_to(as_column(solution_row, gram.shape), gram.shape)[:HIST]


def moved(image, coefficients, column):
    lines = [jnp.sum(coefficients * column(m), axis=0, keepdims=True) for m in range(PARTS)]
    return image + jnp.concatenate(lines, axis=0)


def chosen(x, qt, xs):
    xs[...] = jnp.zeros(xs.shape, F32)
    xs[WIDE : WIDE + PARTS, :] = x
    xs[WIDE + 16 : WIDE + 16 + PARTS, :] = x
    return dot(qt, xs[...].astype(BF16)).astype(BF16)


def far_first_kernel(in_ref, image_ref, upd_ref, qt_ref, send_ref, x_ref, gram_ref, hs, gs, xs):
    right = in_ref[0, 0:1, :]
    hs[0:1, :] = in_ref[0, 1:2, :]
    for i in range(1, 32):
        right = right + in_ref[i, 0:1, :]
        hs[i : i + 1, :] = in_ref[i, 1:2, :]
    half = hs[...]
    gs[pl.ds(0, 32, stride=2), :] = half
    gs[pl.ds(1, 32, stride=2), :] = pltpu.roll(half, WIDE, 1)
    gram = gs[0:COLS, :]
    gram = jnp.where(lanes_of(gram.shape) < WIDE, gram, 0.0)
    gram_ref[...] = gram
    coefficients = solved(gram, right)
    x = moved(image_ref[...], coefficients, lambda m: every(upd_ref, m))
    x_ref[...] = x
    send_ref[...] = chosen(x, qt_ref[...], xs)


def far_next_kernel(in_ref, gram_ref, image_ref, last_ref, upd_ref, qt_ref, send_ref, x_ref, xs):
    total = in_ref[0]
    for i in range(1, 32):
        total = total + in_ref[i]
    gram = gram_ref[...]
    lanes, rows = lanes_of(gram.shape), rows_of(gram.shape)
    new_row = jnp.where(lanes_of(total.shape) < WIDE, pltpu.roll(total, WIDE, 1), 0.0)
    gram = jnp.where(rows == 0, new_row, gram)
    gram = jnp.where(lanes == 0, as_column(new_row, gram.shape), gram)
    coefficients = solved(gram, total)
    image = image_ref[...]
    step = image - last_ref[...]
    first = rows_of((HIST, 128)) == 0
    x = moved(image, coefficients, lambda m: jnp.where(first, step[m : m + 1, :], every(upd_ref, m)))
    for c in range(3):
        x_ref[c] = x[4 * c : 4 * c + 4, :]
    send_ref[...] = chosen(x, qt_ref[...], xs)


def body(
    fluid_load,
    stiffness,
    mapping,
    live_count,
    dest_device,
    local_block,
    compliance,
    start_disp,
    residual_history,
    update_history,
):
    blocks = mapping.shape[0]
    peers = lax.axis_size(FLUID)
    near, far = lax.axis_size(NEAR), lax.axis_size(FAR)
    rows = 8 * peers
    later = 6 * peers
    over_fluid = lambda x: exchange(x.reshape(peers, 3, 2, 128), FLUID).reshape(later, 128)
    parts = lambda a: jnp.swapaxes(a, -3, -2)
    history, updates = (parts(a).reshape(-1, 128) for a in (residual_history, update_history))
    by_part = lambda a: jnp.swapaxes(a, 0, 1).reshape(3 * blocks, 128)
    start = parts(start_disp)[0]
    lines = pltpu.VMEM((3 * blocks, 128), F32)
    square = pltpu.VMEM((128, 128), F32)
    tall = pltpu.VMEM((rows, 128), F32)

    whole, alive = call(
        spread_kernel,
        "spread",
        [((peers, 3, 4, 128), BF16), ((blocks, 128), F32)],
        live_count,
        start,
        in_specs=[SMEM, VMEM],
        cost=pl.CostEstimate(flops=20_000_000_000, bytes_accessed=50_000_000, transcendentals=0),
    )
    whole = exchange(whole, FLUID).reshape(PARTS * peers, 128)
    sent, pick, back, load, stiff, comp, start = call(
        forces_first_kernel,
        "forces_first",
        [
            ((rows, 128), BF16),
            ((3 * blocks, later), BF16),
            ((later, 256), BF16),
            ((3 * blocks, 128), F32),
            ((3 * blocks, 128), F32),
            ((PARTS, 128), F32),
            ((PARTS, 128), F32),
        ],
        alive,
        whole,
        dest_device.reshape(1, blocks),
        local_block.reshape(1, blocks),
        history,
        by_part(fluid_load),
        by_part(stiffness),
        mapping,
        parts(compliance)[0],
        start,
        scratch=[
            pltpu.VMEM((64, 128), F32),
            tall,
            pltpu.VMEM((3 * blocks, PARTS * peers), BF16),
            pltpu.VMEM((rows, 256), BF16),
            lines,
            lines,
        ],
        mib=8,
    )
    got = exchange(sent.reshape(peers, 8, 128), FLUID).reshape(rows, 128)
    line, image, resid, q, qt = call(
        owner_first_kernel,
        "owner_first",
        [((near, 1, 128), F32), ((PARTS, 128), F32), ((PARTS, 128), F32), ((16, later), BF16), ((later, 128), BF16)],
        got,
        comp,
        start,
        history,
        scratch=[tall, square],
        mib=4,
    )
    line = exchange(line, NEAR)
    line = call(near_first_kernel, "near_first", [((far, 2, 128), F32)], line)[0]
    line = exchange(line, FAR)
    sent, x, gram = call(
        far_first_kernel,
        "far_first",
        [((later, 128), BF16), ((PARTS, 128), F32), ((COLS, 128), F32)],
        line,
        image,
        updates,
        qt,
        scratch=[pltpu.VMEM((far, 128), F32), pltpu.VMEM((64, 128), F32), square],
    )
    got = over_fluid(sent)
    sent = call(
        forces_next_kernel,
        "forces_next",
        [((later, 128), BF16)],
        got,
        pick,
        back,
        mapping,
        load,
        stiff,
        scratch=[lines, lines],
        mib=6,
    )[0]
    got = over_fluid(sent)
    last_image = image
    line, image = call(
        owner_next_kernel,
        "owner_next",
        [((near, 1, 128), F32), ((PARTS, 128), F32)],
        got,
        q,
        comp,
        x,
        resid,
        history,
        scratch=[square],
    )
    line = exchange(line, NEAR)
    line = call(near_next_kernel, "near_next", [((far, 1, 128), F32)], line)[0]
    line = exchange(line, FAR)
    sent, struct_disp = call(
        far_next_kernel,
        "far_next",
        [((later, 128), BF16), ((3, 4, 128), F32)],
        line,
        gram,
        image,
        last_image,
        updates,
        qt,
        scratch=[square],
    )
    got = over_fluid(sent)
    final_disp, struct_disp = call(
        final_kernel,
        "final",
        [((3 * blocks, 128), F32), ((3, 4, 128), F32)],
        got,
        pick,
        mapping,
        alive,
        struct_disp,
        scratch=[lines, lines],
        mib=6,
    )
    struct_disp = parts(struct_disp[None])
    return (struct_disp, jnp.swapaxes(final_disp.reshape(3, blocks, 128), 0, 1))


def solution(mesh):
    split = Mesh(mesh.devices.reshape(8, 4, 2, mesh.shape["solid"]), ALL)
    in_specs = (
        P(ALL, None, None),
        P(ALL, None, None),
        P(ALL, None, None),
        P(ALL),
        P(ALL, None),
        P(ALL),
        P("solid", FLUID, None, None),
        P("solid", FLUID, None, None),
        P(None, "solid", FLUID, None, None),
        P(None, "solid", FLUID, None, None),
    )
    out_specs = (P("solid", FLUID, None, None), P(ALL, None, None))
    return jax.shard_map(body, mesh=split, in_specs=in_specs, out_specs=out_specs, check_vma=False)
```

```python
import jax
import jax.numpy as jnp
from jax import lax
from jax.experimental import pallas as pl
from jax.experimental.pallas import tpu as pltpu
from jax.sharding import Mesh
from jax.sharding import PartitionSpec as P

HIST = 50
RIDGE_SHARE = 0.01
ALL = ("z", "x", "c", "solid")
FLUID = ("z", "x", "c")
NEAR = ("c", "solid")
FAR = ("z", "x")
COLS = 56
PARTS = 12
WIDE = 64
F32, BF16 = jnp.float32, jnp.bfloat16
HIGHEST = lax.Precision.HIGHEST
VMEM = pl.BlockSpec(memory_space=pltpu.VMEM)
SMEM = pl.BlockSpec(memory_space=pltpu.SMEM)
HBM = pl.BlockSpec(memory_space=pl.ANY)


def exchange(x, axes):
    return lax.all_to_all(x, axes, split_axis=0, concat_axis=0, tiled=True)


def call(kernel, name, outs, *args, in_specs=None, out_specs=None, scratch=(), mib=2, cost=None):
    return pl.pallas_call(
        kernel,
        out_shape=[jax.ShapeDtypeStruct(shape, dtype) for shape, dtype in outs],
        compiler_params=pltpu.CompilerParams(vmem_limit_bytes=mib << 20),
        in_specs=in_specs or [VMEM] * len(args),
        out_specs=out_specs or [VMEM] * len(outs),
        scratch_shapes=list(scratch),
        cost_estimate=cost,
        name=name,
    )(*args)


def dot(a, b, dims=((1,), (0,)), precision=None):
    return lax.dot_general(a, b, (dims, ((), ())), precision=precision, preferred_element_type=F32)


def lanes_of(shape):
    return lax.broadcasted_iota(jnp.int32, shape, len(shape) - 1)


def rows_of(shape):
    return lax.broadcasted_iota(jnp.int32, shape, 0)


def every(ref, part):
    return ref[pl.ds(part, HIST, stride=PARTS), :]


def as_column(row, shape):
    on_diag = lanes_of(shape) == rows_of(shape)
    return jnp.sum(jnp.where(on_diag, row, jnp.zeros_like(row)), axis=1, keepdims=True)


def sixths(i):
    peer = jnp.floor((i.astype(F32) + 0.5) * (1.0 / 6.0)).astype(jnp.int32)
    row = i - 6 * peer
    return peer, row // 2, row % 2


def spread_kernel(live_ref, x_ref, out_ref, alive_ref):
    out_ref[...] = jnp.broadcast_to(x_ref[...].astype(BF16)[None], out_ref.shape)
    alive_ref[...] = jnp.where(rows_of(alive_ref.shape) < live_ref[0], 1.0, 0.0)


def forces_first_kernel(
    alive_ref, x_ref, dest_ref, local_ref, hist_ref, raw_load_ref, raw_stiff_ref, map_ref, comp_ref, start_ref,
    out_ref, pick_ref, back_ref, load_ref, stiff_ref, flat_comp_ref, flat_start_ref, gs, ss, whole_ref, back_first_ref, xs, us,
):
    for c in range(3):
        flat_comp_ref[4 * c : 4 * c + 4, :] = comp_ref[c]
        flat_start_ref[4 * c : 4 * c + 4, :] = start_ref[c]
    square = (64, 128)
    lanes, rows = lanes_of(square), rows_of(square)
    dest = jnp.where(lanes < 64, jnp.concatenate([dest_ref[...]] * 2, axis=1), -1)
    local = jnp.concatenate([local_ref[...]] * 2, axis=1)
    dest_column = as_column(dest.astype(F32), square)
    local_column = as_column(local.astype(F32), square).astype(jnp.int32)
    same = (dest_column == dest.astype(F32)) & (lanes < 64)
    dest_column = dest_column.astype(jnp.int32)
    slot_column = jnp.sum(jnp.where(same & (lanes < rows), 1.0, 0.0), axis=1, keepdims=True)
    slot_row = jnp.sum(jnp.where(same & (rows < lanes), 1.0, 0.0), axis=0, keepdims=True)
    slot_column = slot_column.astype(jnp.int32)
    place_row = dest[0:1] * 8 + slot_row.astype(jnp.int32) * 4
    wide = lanes_of((64, 384))
    wider = lanes_of((64, 768))
    for c in range(3):
        pick_ref[64 * c : 64 * c + 64, :] = jnp.where(wide == dest_column * 6 + 2 * c + slot_column, 1.0, 0.0).astype(BF16)
        whole_column = dest_column * PARTS + 4 * c + local_column
        whole_ref[64 * c : 64 * c + 64, :] = jnp.where(wider == whole_column, 1.0, 0.0).astype(BF16)
    low = lanes[0:1] < 64
    place_next = dest[0:1] * 6 + slot_row.astype(jnp.int32)
    for place, step, ref in ((place_row, 1, back_first_ref), (place_next, 2, back_ref)):
        tall = rows_of((ref.shape[0], 128))
        first = jnp.where(low, place, pltpu.roll(place, 64, 1) + step)
        second = jnp.where(low, place + 2 * step, -1)
        ref[:, 0:128] = jnp.where(tall == first, 1.0, 0.0).astype(BF16)
        ref[:, 128:256] = jnp.where(tall == second, 1.0, 0.0).astype(BF16)
    part = lanes % 16
    held = (lanes >= 64) & (lanes // 16 - 4 == slot_column) & (part % 4 == local_column) & (part < PARTS)
    onto = jnp.where(dest == rows, 1.0, 0.0).astype(BF16)
    marks = dot(onto[:, 0:64], jnp.where(held, 1.0, 0.0).astype(BF16))
    history = jnp.concatenate([every(hist_ref, m) for m in range(PARTS)], axis=1)
    gs[...] = jnp.zeros(square, F32)
    gs[0:HIST, 0:HIST] = dot(history, history, ((1,), (1,)), HIGHEST)
    gram = gs[...]
    high = gram.astype(BF16).astype(F32)
    middle = (gram - high).astype(BF16).astype(F32)
    low_part = gram - high - middle
    ss[...] = jnp.zeros((512, 128), F32)
    ss[pl.ds(3, 64, stride=8), :] = high + pltpu.roll(middle, WIDE, 1)
    ss[pl.ds(7, 64, stride=8), :] = low_part + marks
    alive = alive_ref[...]
    for c in range(3):
        load_ref[64 * c : 64 * c + 64, :] = raw_load_ref[64 * c : 64 * c + 64, :] * alive
        stiff_ref[64 * c : 64 * c + 64, :] = raw_stiff_ref[64 * c : 64 * c + 64, :] * alive
    filled = forces(x_ref, whole_ref, back_first_ref, map_ref, load_ref, stiff_ref, xs, us)
    out_ref[...] = (filled + ss[...]).astype(BF16)


def apply_maps(map_ref, from_ref, to_ref, dims, blocks=range(0, 64, 2)):
    for b in blocks:
        first, second = pl.ds(b, 3, stride=64), pl.ds(b + 1, 3, stride=64)
        both = jnp.concatenate([from_ref[first, :], from_ref[second, :]], axis=0).astype(BF16)
        if dims == ((1,), (0,)):
            maps = jnp.concatenate([map_ref[b], map_ref[b + 1]], axis=1)
        else:
            maps = map_ref[b : b + 2].reshape(256, 128)
        out = dot(both, maps, dims)
        to_ref[first, :] = out[0:3, 0:128]
        to_ref[second, :] = out[3:6, 128:256]


def forces(x_ref, pick_ref, back_ref, map_ref, load_ref, stiff_ref, xs, us):
    xs[...] = dot(pick_ref[...], x_ref[...])
    apply_maps(map_ref, xs, us, ((1,), (0,)))
    xs[...] = load_ref[...] - stiff_ref[...] * us[...]
    apply_maps(map_ref, xs, us, ((1,), (1,)))
    contrib = jnp.concatenate([us[...].astype(BF16), jnp.zeros((64, 128), BF16)], axis=0)
    return dot(back_ref[...], contrib)


def forces_next_kernel(x_ref, pick_ref, back_ref, map_ref, load_ref, stiff_ref, out_ref, xs, us):
    out_ref[...] = forces(x_ref, pick_ref, back_ref, map_ref, load_ref, stiff_ref, xs, us).astype(BF16)


def final_kernel(x_ref, pick_ref, map_ref, alive_ref, struct_ref, out_ref, disp_ref, xs, us, done, sems):
    copies = [pltpu.make_async_copy(struct_ref, disp_ref, sems.at[6])]
    copies[0].start()
    xs[...] = dot(pick_ref[...], x_ref[...])
    for half in range(2):
        apply_maps(map_ref, xs, us, ((1,), (0,)), range(32 * half, 32 * half + 32, 2))
        for c in range(3):
            rows = pl.ds(64 * c + 32 * half, 32)
            done[rows, :] = us[rows, :] * alive_ref[32 * half : 32 * half + 32, :]
            copies.append(pltpu.make_async_copy(done.at[rows, :], out_ref.at[rows, :], sems.at[3 * half + c]))
            copies[-1].start()
    for copy in copies:
        copy.wait()


def history_sums(hist_ref, vector):
    acc = every(hist_ref, 0) * vector[0:1, :]
    for m in range(1, PARTS):
        acc = acc + every(hist_ref, m) * vector[m : m + 1, :]
    return acc


def as_row(scratch, first, second):
    scratch[...] = jnp.zeros(scratch.shape, F32)
    scratch[0:HIST, :] = first
    if second is not None:
        scratch[WIDE : WIDE + HIST, :] = second
    return dot(jnp.ones((8, 128), F32), scratch[...], ((1,), (1,)), HIGHEST)[0:1, :]


def owner_first_kernel(got_ref, comp_ref, x_ref, hist_ref, msg_ref, image_ref, resid_ref, q_ref, qt_ref, xs, hs):
    got = got_ref[...]
    xs[...] = got.astype(F32)
    mark3 = xs[pl.ds(3, 64, stride=8), :]
    mark7 = xs[pl.ds(7, 64, stride=8), :]
    sum3 = jnp.sum(mark3, axis=0, keepdims=True)
    sum7 = jnp.sum(mark7, axis=0, keepdims=True)
    gram_row = sum3 + pltpu.roll(sum3, WIDE, 1) + pltpu.roll(sum7, WIDE, 1)
    spread = jnp.where(lanes_of((64, 512)) // 8 == rows_of((64, 512)), 1.0, 0.0).astype(BF16)
    wide = dot(mark7.astype(BF16), spread, ((0,), (0,)))
    part = rows_of((16, 512))
    row = lanes_of((16, 512)) % 8
    match = (part // 4 == row % 4) & (part < PARTS)
    q = jnp.where(match & (row < 4), wide[64:80], 0.0)
    q = (q + jnp.where(match & (row >= 4), wide[80:96], 0.0)).astype(BF16)
    peer, component, place = sixths(lanes_of((64, 384)))
    spread = jnp.where(peer == rows_of((64, 384)), 1.0, 0.0).astype(BF16)
    wide = dot(mark7.astype(BF16), spread, ((0,), (0,)))
    part = rows_of((16, 384))
    match = (part // 4 == component[0:16]) & (part < PARTS)
    later = jnp.where(match & (place[0:16] == 0), wide[64:80], 0.0)
    q_ref[...] = (later + jnp.where(match & (place[0:16] == 1), wide[80:96], 0.0)).astype(BF16)
    peer, component, place = sixths(rows_of((384, 128)))
    lane = lanes_of((384, 128))
    spread = jnp.where(peer == lane, 1.0, 0.0).astype(BF16)
    tall = dot(spread[:, 0:64], mark7.astype(BF16))
    match = ((lane % 16) // 4 == component) & (lane // 16 - 4 == place) & (lane % 16 < PARTS)
    qt_ref[...] = jnp.where(match, tall, 0.0).astype(BF16)
    image = comp_ref[...] * dot(q, got)[0:PARTS]
    resid = image - x_ref[...]
    image_ref[...] = image
    resid_ref[...] = resid
    line = as_row(hs, history_sums(hist_ref, resid), None)
    line = jnp.where(lanes_of(line.shape) < WIDE, line, gram_row)
    msg_ref[...] = jnp.broadcast_to(line.reshape(1, 1, 128), msg_ref.shape)


def owner_next_kernel(got_ref, q_ref, comp_ref, x_ref, last_ref, hist_ref, msg_ref, image_ref, hs):
    image = comp_ref[...] * dot(q_ref[...], got_ref[...])[0:PARTS]
    image_ref[...] = image
    resid = image - x_ref[...]
    newest = resid - last_ref[...]
    first = rows_of((HIST, 128)) == 0
    own_right = jnp.sum(newest * resid, axis=0, keepdims=True)
    own_row = jnp.sum(newest * newest, axis=0, keepdims=True)
    right = jnp.where(first, own_right, history_sums(hist_ref, resid))
    row = jnp.where(first, own_row, history_sums(hist_ref, newest))
    line = as_row(hs, right, row)
    msg_ref[...] = jnp.broadcast_to(line.reshape(1, 1, 128), msg_ref.shape)


def near_first_kernel(in_ref, out_ref):
    sums = []
    for c in range(2):
        total = in_ref[8 * c]
        for y in range(1, 8):
            total = total + in_ref[8 * c + y]
        sums.append(total)
    right = sums[0] + sums[1]
    rows = jnp.where(lanes_of((1, 128)) < WIDE, pltpu.roll(sums[0], WIDE, 1), sums[1])
    both = jnp.concatenate([right, rows], axis=0)
    out_ref[...] = jnp.broadcast_to(both[None], out_ref.shape)


def near_next_kernel(in_ref, out_ref):
    total = in_ref[0]
    for i in range(1, in_ref.shape[0]):
        total = total + in_ref[i]
    out_ref[...] = jnp.broadcast_to(total[None], out_ref.shape)


def solved(gram, right):
    lanes, rows = lanes_of(gram.shape), rows_of(gram.shape)
    diag = (rows == lanes) & (rows < HIST)
    trace = jnp.sum(jnp.sum(jnp.where(diag, gram, 0.0), axis=1, keepdims=True), axis=0, keepdims=True)
    scale = 1.0 / trace
    a = gram * scale + jnp.where(diag, RIDGE_SHARE / HIST, 0.0)
    a = jnp.where(lanes == rows + WIDE, 1.0, a)
    under = jnp.where(lanes_of(right.shape) < WIDE, right * scale, 0.0)
    tiles = [a[8 * i : 8 * i + 8] for i in range(COLS // 8)] + [jnp.broadcast_to(under, (8, 128))]
    spread = lambda k, start: [jnp.broadcast_to(tile[:, k : k + 1], (8, 128)) for tile in tiles[start:]]
    lefts, rights = spread(0, 0), spread(1, 0)
    for k in range(0, HIST, 2):
        first = k // 8
        at = lambda stack, j: stack[j // 8 - first][j % 8 : j % 8 + 1]
        coming = [(j, spread(j, first)) for j in (k + 2, k + 3) if j < HIST]
        p11, p12, p21, p22 = at(lefts, k), at(rights, k), at(lefts, k + 1), at(rights, k + 1)
        inverse = 1.0 / (p11 * p22 - p12 * p21)

        def scaled(one, two):
            return (p22 * one - p12 * two) * inverse, (p11 * two - p21 * one) * inverse

        def reduced(stack, new1, new2):
            return [v - left * new1 - right * new2 for v, left, right in zip(stack, lefts, rights)]

        following = [reduced(old, *scaled(at(lefts, j), at(rights, j))) for j, old in coming]
        tiles[first:] = reduced(tiles[first:], *scaled(at(tiles[first:], k), at(tiles[first:], k + 1)))
        if following:
            lefts, rights = (stack[(k + 2) // 8 - first :] for stack in following)
    solution_row = pltpu.roll(tiles[-1], WIDE, 1)[0:1]
    return jnp.broadcast_to(as_column(solution_row, gram.shape), gram.shape)[:HIST]


def moved(image, coefficients, column):
    lines = [jnp.sum(coefficients * column(m), axis=0, keepdims=True) for m in range(PARTS)]
    return image + jnp.concatenate(lines, axis=0)


def chosen(x, qt, xs):
    xs[...] = jnp.zeros(xs.shape, F32)
    xs[WIDE : WIDE + PARTS, :] = x
    xs[WIDE + 16 : WIDE + 16 + PARTS, :] = x
    return dot(qt, xs[...].astype(BF16)).astype(BF16)


def far_first_kernel(in_ref, image_ref, upd_ref, qt_ref, send_ref, x_ref, gram_ref, hs, gs, xs):
    right = in_ref[0, 0:1, :]
    hs[0:1, :] = in_ref[0, 1:2, :]
    for i in range(1, 32):
        right = right + in_ref[i, 0:1, :]
        hs[i : i + 1, :] = in_ref[i, 1:2, :]
    half = hs[...]
    gs[pl.ds(0, 32, stride=2), :] = half
    gs[pl.ds(1, 32, stride=2), :] = pltpu.roll(half, WIDE, 1)
    gram = gs[0:COLS, :]
    gram = jnp.where(lanes_of(gram.shape) < WIDE, gram, 0.0)
    gram_ref[...] = gram
    coefficients = solved(gram, right)
    x = moved(image_ref[...], coefficients, lambda m: every(upd_ref, m))
    x_ref[...] = x
    send_ref[...] = chosen(x, qt_ref[...], xs)


def far_next_kernel(in_ref, gram_ref, image_ref, last_ref, upd_ref, qt_ref, send_ref, x_ref, xs):
    total = in_ref[0]
    for i in range(1, 32):
        total = total + in_ref[i]
    gram = gram_ref[...]
    lanes, rows = lanes_of(gram.shape), rows_of(gram.shape)
    new_row = jnp.where(lanes_of(total.shape) < WIDE, pltpu.roll(total, WIDE, 1), 0.0)
    gram = jnp.where(rows == 0, new_row, gram)
    gram = jnp.where(lanes == 0, as_column(new_row, gram.shape), gram)
    coefficients = solved(gram, total)
    image = image_ref[...]
    step = image - last_ref[...]
    first = rows_of((HIST, 128)) == 0
    x = moved(image, coefficients, lambda m: jnp.where(first, step[m : m + 1, :], every(upd_ref, m)))
    for c in range(3):
        x_ref[c] = x[4 * c : 4 * c + 4, :]
    send_ref[...] = chosen(x, qt_ref[...], xs)


def body(
    fluid_load,
    stiffness,
    mapping,
    live_count,
    dest_device,
    local_block,
    compliance,
    start_disp,
    residual_history,
    update_history,
):
    blocks = mapping.shape[0]
    peers = lax.axis_size(FLUID)
    near, far = lax.axis_size(NEAR), lax.axis_size(FAR)
    rows = 8 * peers
    later = 6 * peers
    over_fluid = lambda x: exchange(x.reshape(peers, 3, 2, 128), FLUID).reshape(later, 128)
    parts = lambda a: jnp.swapaxes(a, -3, -2)
    history, updates = (parts(a).reshape(-1, 128) for a in (residual_history, update_history))
    by_part = lambda a: jnp.swapaxes(a, 0, 1).reshape(3 * blocks, 128)
    start = parts(start_disp)[0]
    lines = pltpu.VMEM((3 * blocks, 128), F32)
    square = pltpu.VMEM((128, 128), F32)
    tall = pltpu.VMEM((rows, 128), F32)

    whole, alive = call(
        spread_kernel,
        "spread",
        [((peers, 3, 4, 128), BF16), ((blocks, 128), F32)],
        live_count,
        start,
        in_specs=[SMEM, VMEM],
        cost=pl.CostEstimate(flops=20_000_000_000, bytes_accessed=50_000_000, transcendentals=0),
    )
    whole = exchange(whole, FLUID).reshape(PARTS * peers, 128)
    sent, pick, back, load, stiff, comp, start = call(
        forces_first_kernel,
        "forces_first",
        [
            ((rows, 128), BF16),
            ((3 * blocks, later), BF16),
            ((later, 256), BF16),
            ((3 * blocks, 128), F32),
            ((3 * blocks, 128), F32),
            ((PARTS, 128), F32),
            ((PARTS, 128), F32),
        ],
        alive,
        whole,
        dest_device.reshape(1, blocks),
        local_block.reshape(1, blocks),
        history,
        by_part(fluid_load),
        by_part(stiffness),
        mapping,
        parts(compliance)[0],
        start,
        scratch=[
            pltpu.VMEM((64, 128), F32),
            tall,
            pltpu.VMEM((3 * blocks, PARTS * peers), BF16),
            pltpu.VMEM((rows, 256), BF16),
            lines,
            lines,
        ],
        mib=8,
    )
    got = exchange(sent.reshape(peers, 8, 128), FLUID).reshape(rows, 128)
    line, image, resid, q, qt = call(
        owner_first_kernel,
        "owner_first",
        [((near, 1, 128), F32), ((PARTS, 128), F32), ((PARTS, 128), F32), ((16, later), BF16), ((later, 128), BF16)],
        got,
        comp,
        start,
        history,
        scratch=[tall, square],
        mib=4,
    )
    line = exchange(line, NEAR)
    line = call(near_first_kernel, "near_first", [((far, 2, 128), F32)], line)[0]
    line = exchange(line, FAR)
    sent, x, gram = call(
        far_first_kernel,
        "far_first",
        [((later, 128), BF16), ((PARTS, 128), F32), ((COLS, 128), F32)],
        line,
        image,
        updates,
        qt,
        scratch=[pltpu.VMEM((far, 128), F32), pltpu.VMEM((64, 128), F32), square],
    )
    got = over_fluid(sent)
    sent = call(
        forces_next_kernel,
        "forces_next",
        [((later, 128), BF16)],
        got,
        pick,
        back,
        mapping,
        load,
        stiff,
        scratch=[lines, lines],
        mib=6,
    )[0]
    got = over_fluid(sent)
    last_image = image
    line, image = call(
        owner_next_kernel,
        "owner_next",
        [((near, 1, 128), F32), ((PARTS, 128), F32)],
        got,
        q,
        comp,
        x,
        resid,
        history,
        scratch=[square],
    )
    line = exchange(line, NEAR)
    line = call(near_next_kernel, "near_next", [((far, 1, 128), F32)], line)[0]
    line = exchange(line, FAR)
    sent, struct_disp = call(
        far_next_kernel,
        "far_next",
        [((later, 128), BF16), ((3, 4, 128), F32)],
        line,
        gram,
        image,
        last_image,
        updates,
        qt,
        scratch=[square],
    )
    got = over_fluid(sent)
    final_disp, struct_disp = call(
        final_kernel,
        "final",
        [((3 * blocks, 128), F32), ((3, 4, 128), F32)],
        got,
        pick,
        mapping,
        alive,
        struct_disp,
        out_specs=[HBM, HBM],
        scratch=[lines, lines, lines, pltpu.SemaphoreType.DMA((7,))],
        mib=6,
    )
    struct_disp = parts(struct_disp[None])
    return (struct_disp, jnp.swapaxes(final_disp.reshape(3, blocks, 128), 0, 1))


def solution(mesh):
    split = Mesh(mesh.devices.reshape(8, 4, 2, mesh.shape["solid"]), ALL)
    in_specs = (
        P(ALL, None, None),
        P(ALL, None, None),
        P(ALL, None, None),
        P(ALL),
        P(ALL, None),
        P(ALL),
        P("solid", FLUID, None, None),
        P("solid", FLUID, None, None),
        P(None, "solid", FLUID, None, None),
        P(None, "solid", FLUID, None, None),
    )
    out_specs = (P("solid", FLUID, None, None), P(ALL, None, None))
    return jax.shard_map(body, mesh=split, in_specs=in_specs, out_specs=out_specs, check_vma=False)
```
